64 devices in a mesh: dp: 4 (over x, y), sp: 16 (over z, core).
Axes of the slice: x: 2, y: 2, z: 8, core: 2. Of those that a mesh axis runs over, the one named last changes fastest.
The devices are a block of a 4x4x8 slice.
Arguments:
- hidden: bfloat16 [192, 4096], P('dp'), parts along dimension 0
- ln_gamma: float32 [4096], replicated
- ln_beta: float32 [4096], replicated
- w_qkv: bfloat16 [4096, 4608], replicated
- w_out: bfloat16 [4096, 4096], replicated
- w_up: bfloat16 [4096, 16384], P(None, 'sp')
- w_down: bfloat16 [16384, 4096], P('sp')
- k_cache: bfloat16 [192, 2048, 256], P('dp', 'sp'), parts along dimension 0
- v_cache: bfloat16 [192, 2048, 256], P('dp', 'sp'), parts along dimension 0
- positions: int32 [192], P('dp'), parts along dimension 0
Outputs:
- output 1: bfloat16 [192, 4096], P('dp'), parts along dimension 0
- output 2: bfloat16 [192, 2048, 256], P('dp', 'sp'), parts along dimension 0
- output 3: bfloat16 [192, 2048, 256], P('dp', 'sp'), parts along dimension 0
There are 4 independent parts. The reference program is written for one: setup_inputs(seed, part) draws one part's arguments, and reference() takes and returns one part's arrays. A program takes and returns all parts, laid end to end along the dimension named above; an argument that names none is the same for every part.
All inputs are finite; a program needn't handle non-finite values.
Results may differ from the reference program's by a relative error of at most 0.00517107.
Values sent between devices are 32-bit elements.
A program may use at most 768 MiB of HBM per device.

```python
import jax
import jax.numpy as jnp
from jax import lax

BATCH_ROWS = 48
D_MODEL = 4096
N_HEADS = 16
HEAD_DIM = 256
FF_DIM = 16384
SEQ_SHARD = 128
N_SHARDS = 16
SEQ_LEN = N_SHARDS * SEQ_SHARD
LN_EPS = 1e-5
ROPE_BASE = 10000.0
NEG_FILL = -1e30


def setup_inputs(seed: int = 0, part: int = 0) -> dict:
    base_key = jax.random.key(seed)
    weight_keys = jax.random.split(base_key, 6)
    part_keys = jax.random.split(jax.random.fold_in(base_key, part), 4)
    hidden = jax.random.normal(part_keys[0], (BATCH_ROWS, D_MODEL), jnp.float32).astype(jnp.bfloat16)
    ln_gamma = 1.0 + 0.3 * jax.random.normal(weight_keys[0], (D_MODEL,), jnp.float32)
    ln_beta = 0.3 * jax.random.normal(weight_keys[1], (D_MODEL,), jnp.float32)
    w_qkv = (jax.random.normal(weight_keys[2], (D_MODEL, (N_HEADS + 2) * HEAD_DIM), jnp.float32) * D_MODEL ** -0.5).astype(jnp.bfloat16)
    out_scale = 0.5 * SEQ_LEN ** 0.5 * (N_HEADS * HEAD_DIM) ** -0.5
    w_out = (jax.random.normal(weight_keys[3], (N_HEADS * HEAD_DIM, D_MODEL), jnp.float32) * out_scale).astype(jnp.bfloat16)
    w_up = (jax.random.normal(weight_keys[4], (D_MODEL, FF_DIM), jnp.float32) * D_MODEL ** -0.5).astype(jnp.bfloat16)
    w_down = (jax.random.normal(weight_keys[5], (FF_DIM, D_MODEL), jnp.float32) * FF_DIM ** -0.5).astype(jnp.bfloat16)
    k_cache = jax.random.normal(part_keys[1], (BATCH_ROWS, SEQ_LEN, HEAD_DIM), jnp.float32).astype(jnp.bfloat16)
    v_cache = jax.random.normal(part_keys[2], (BATCH_ROWS, SEQ_LEN, HEAD_DIM), jnp.float32).astype(jnp.bfloat16)
    positions = jax.random.randint(part_keys[3], (BATCH_ROWS,), SEQ_LEN // 2, SEQ_LEN, dtype=jnp.int32)
    positions = positions.at[0].set(SEQ_LEN - 1).at[1].set(SEQ_LEN // 2)
    return {'hidden': hidden, 'ln_gamma': ln_gamma, 'ln_beta': ln_beta, 'w_qkv': w_qkv, 'w_out': w_out, 'w_up': w_up, 'w_down': w_down, 'k_cache': k_cache, 'v_cache': v_cache, 'positions': positions}


def layer_norm(hidden, ln_gamma, ln_beta):
    hidden_f32 = hidden.astype(jnp.float32)
    row_mean = jnp.mean(hidden_f32, axis=-1, keepdims=True)
    centered = hidden_f32 - row_mean
    row_var = jnp.mean(centered * centered, axis=-1, keepdims=True)
    return (centered * lax.rsqrt(row_var + LN_EPS) * ln_gamma + ln_beta).astype(jnp.bfloat16)


def rotary_tables(positions, head_dim):
    inv_freq = 1.0 / (ROPE_BASE ** (jnp.arange(0, head_dim, 2, dtype=jnp.float32) / head_dim))
    angles = positions.astype(jnp.float32)[:, None] * inv_freq[None, :]
    cos_half = jnp.cos(angles)
    sin_half = jnp.sin(angles)
    return jnp.concatenate([cos_half, cos_half], axis=-1), jnp.concatenate([sin_half, sin_half], axis=-1)


def apply_rotary(vecs, cos_full, sin_full):
    vecs_f32 = vecs.astype(jnp.float32)
    half_dim = vecs.shape[-1] // 2
    rotated = jnp.concatenate([-vecs_f32[..., half_dim:], vecs_f32[..., :half_dim]], axis=-1)
    return (vecs_f32 * cos_full + rotated * sin_full).astype(jnp.bfloat16)


def row_attention(row_inputs):
    q_row, k_row, v_row, pos_row = row_inputs
    scores = jnp.dot(q_row, k_row.T, preferred_element_type=jnp.float32) * HEAD_DIM ** -0.5
    scores = scores.reshape(N_HEADS, N_SHARDS, SEQ_SHARD)
    valid_mask = (jnp.arange(SEQ_LEN) <= pos_row).reshape(N_SHARDS, SEQ_SHARD)
    masked = jnp.where(valid_mask, scores, NEG_FILL)
    block_max = jnp.max(masked, axis=-1)
    exp_scores = jnp.where(valid_mask, jnp.exp(masked - block_max[..., None]), 0.0)
    block_sum = jnp.sum(exp_scores, axis=-1)
    block_ctx = jnp.einsum('hcs,csd->hcd', exp_scores.astype(jnp.bfloat16).astype(jnp.float32), v_row.reshape(N_SHARDS, SEQ_SHARD, HEAD_DIM).astype(jnp.float32))
    top_max = jnp.max(block_max, axis=-1)
    scale_w = jnp.exp(block_max - top_max[:, None])
    total_sum = jnp.sum(block_sum * scale_w, axis=-1)
    total_ctx = jnp.sum(block_ctx * scale_w[..., None], axis=1)
    return (total_ctx / total_sum[:, None]).astype(jnp.bfloat16)


def reference(hidden, ln_gamma, ln_beta, w_qkv, w_out, w_up, w_down, k_cache, v_cache, positions):
    normed = layer_norm(hidden, ln_gamma, ln_beta)
    qkv_proj = jnp.dot(normed, w_qkv, preferred_element_type=jnp.float32).astype(jnp.bfloat16)
    qkv_proj = qkv_proj.reshape(BATCH_ROWS, N_HEADS + 2, HEAD_DIM)
    cos_full, sin_full = rotary_tables(positions, HEAD_DIM)
    q_rot = apply_rotary(qkv_proj[:, :N_HEADS], cos_full[:, None, :], sin_full[:, None, :])
    k_rot = apply_rotary(qkv_proj[:, N_HEADS], cos_full, sin_full)
    v_new = qkv_proj[:, N_HEADS + 1]
    write_mask = (jnp.arange(SEQ_LEN)[None, :] == positions[:, None])[:, :, None]
    k_next = jnp.where(write_mask, k_rot[:, None, :], k_cache)
    v_next = jnp.where(write_mask, v_new[:, None, :], v_cache)
    context = lax.map(row_attention, (q_rot, k_next, v_next, positions))
    attn_out = jnp.dot(context.reshape(BATCH_ROWS, N_HEADS * HEAD_DIM), w_out, preferred_element_type=jnp.float32)
    up_proj = jnp.dot(normed, w_up, preferred_element_type=jnp.float32)
    activated = jax.nn.gelu(up_proj, approximate=False).astype(jnp.bfloat16)
    mlp_out = jnp.dot(activated, w_down, preferred_element_type=jnp.float32)
    out_hidden = (hidden.astype(jnp.float32) + attn_out + mlp_out).astype(jnp.bfloat16)
    return (out_hidden, k_next, v_next)
```

```python
import functools

import jax
import jax.numpy as jnp
from jax import lax
from jax.experimental import pallas as pl
from jax.experimental.pallas import tpu as pltpu
from jax.sharding import PartitionSpec as P

LN_EPS = 1e-5
ROPE_BASE = 10000.0
NEG_FILL = -1e30
MESH = pl.DeviceIdType.MESH
BLK = 256
HALF = 128
F32 = jnp.float32
BF16 = jnp.bfloat16


def rotary_tables(positions, head_dim):
    inv_freq = 1.0 / (ROPE_BASE ** (jnp.arange(0, head_dim, 2, dtype=F32) / head_dim))
    angles = positions.astype(F32)[:, None] * inv_freq[None, :]
    return jnp.cos(angles), jnp.sin(angles)


def layer_kernel(chips, heads, x_hbm, gamma_hbm, beta_hbm, wqkv_hbm, wout_hbm, wup_hbm, wdown_hbm, k_hbm, v_hbm,
                 cos_ref, sin_ref, lp_ref,
                 out_ref, knew_ref, vnew_ref,
                 x_s, gb_s, h_s, act_s, w_s, k_s, v_s, qk_s, ps_s, pr_s, ss_s, rs_s, ma_s, ost_s, orx_s, cz_s, r_s, g_s, acc_s,
                 in_sem, up_sem, dn_sem, qkv_sem, kv_sem, wo_sem,
                 pd_send, pd_recv, rs_send, rs_recv, ma_send, ma_fsend, ma_recv,
                 qx_send, qx_recv, st_send, st_recv, aa_send, aa_recv, cg_send, cg_fsend, cg_recv):
    rows, d_model = x_hbm.shape
    ff = wup_hbm.shape[1]
    seq = k_hbm.shape[1]
    n_up = ff // BLK
    n_col = d_model // BLK
    half_heads = heads // 2
    slots = (heads + 2) // 2
    tail = rows + 8
    up_rows, dn_rows = d_model, ff
    dn_base = n_up * up_rows
    qkv_base = dn_base + n_col * dn_rows
    n_kv = kv_sem.shape[1]
    kv_rows = rows // n_kv

    s = lax.axis_index('sp')
    z = lax.div(s, 2)
    c = lax.rem(s, 2)
    pc = 1 - c
    partner = {'sp': 2 * z + pc}

    def chip(k):
        return lax.rem(z + k, chips)

    def peer(zz):
        return {'sp': 2 * zz + c}

    def order(i):
        return chip(i + chips // 2)

    def in_copy(i):
        src, dst = ((x_hbm, x_s), (gamma_hbm, gb_s.at[pl.ds(0, 1)]), (beta_hbm, gb_s.at[pl.ds(8, 1)]))[i]
        return pltpu.make_async_copy(src, dst, in_sem.at[i])

    def up_copy(i):
        col = pl.multiple_of(i * BLK, BLK)
        row = pl.multiple_of(i * up_rows, BLK)
        return pltpu.make_async_copy(wup_hbm.at[:, pl.ds(col, BLK)], w_s.at[pl.ds(row, up_rows)], up_sem.at[i])

    def dn_copy(half, i):
        owner = pc if half == 0 else c
        col = pl.multiple_of((owner * chips + order(i)) * BLK, BLK)
        slot = half * chips + i
        row = pl.multiple_of(dn_base + slot * dn_rows, BLK)
        return pltpu.make_async_copy(wdown_hbm.at[:, pl.ds(col, BLK)], w_s.at[pl.ds(row, dn_rows)], dn_sem.at[slot])

    def qkv_copy(i):
        col = pl.multiple_of((c * slots + i) * BLK, BLK)
        row = pl.multiple_of(qkv_base + i * d_model, BLK)
        return pltpu.make_async_copy(wqkv_hbm.at[:, pl.ds(col, BLK)], w_s.at[pl.ds(row, d_model)], qkv_sem.at[i])

    def kv_copy(t, i):
        src, dst = ((k_hbm, k_s), (v_hbm, v_s))[t]
        sl = pl.ds(i * kv_rows, kv_rows)
        return pltpu.make_async_copy(src.at[sl], dst.at[sl], kv_sem.at[t, i])

    def wo_copy(i):
        col = pl.multiple_of(i * BLK, BLK)
        row = pl.multiple_of(i * d_model, BLK)
        return pltpu.make_async_copy(wout_hbm.at[:, pl.ds(col, BLK)], w_s.at[pl.ds(row, d_model)], wo_sem.at[i])

    def pd_copy(zz):
        return pltpu.make_async_remote_copy(ps_s.at[zz], pr_s.at[zz], pd_send.at[zz], pd_recv.at[zz], device_id=partner, device_id_type=MESH)

    def rs_copy(dst, src):
        return pltpu.make_async_remote_copy(ss_s.at[dst], rs_s.at[src], rs_send.at[dst], rs_recv.at[src], device_id=peer(dst), device_id_type=MESH)

    def ma_copy(dst, src):
        slot = c * chips + src
        return pltpu.make_async_remote_copy(ma_s.at[slot], ma_s.at[slot], ma_send.at[dst], ma_recv.at[slot], device_id=peer(dst), device_id_type=MESH)

    def ma_fwd(owner, zz):
        slot = owner * chips + zz
        return pltpu.make_async_remote_copy(ma_s.at[slot], ma_s.at[slot], ma_fsend.at[zz], ma_recv.at[slot], device_id=partner, device_id_type=MESH)

    def qx_copy(owner, i):
        row = pl.multiple_of((owner * slots + i) * 2 * rows, 8)
        ref = qk_s.at[pl.ds(row, 2 * rows)]
        return pltpu.make_async_remote_copy(ref, ref, qx_send.at[i], qx_recv.at[i], device_id=partner, device_id_type=MESH)

    def st_copy():
        return pltpu.make_async_remote_copy(ost_s.at[pc], orx_s, st_send.at[0], st_recv.at[0], device_id=partner, device_id_type=MESH)

    def aa_copy(dst, src):
        a = cz_s.at[pl.ds(pl.multiple_of(dst * 2 * tail, 8), 2 * tail)]
        b = r_s.at[pl.ds(pl.multiple_of(src * 2 * tail, 8), 2 * tail)]
        return pltpu.make_async_remote_copy(a, b, aa_send.at[dst], aa_recv.at[src], device_id=peer(dst), device_id_type=MESH)

    def cg_copy(dst, src):
        slot = c * chips + src
        return pltpu.make_async_remote_copy(g_s.at[slot], g_s.at[slot], cg_send.at[dst], cg_recv.at[slot], device_id=peer(dst), device_id_type=MESH)

    def cg_fwd(owner, zz):
        slot = owner * chips + zz
        return pltpu.make_async_remote_copy(g_s.at[slot], g_s.at[slot], cg_fsend.at[zz], cg_recv.at[slot], device_id=partner, device_id_type=MESH)

    for i in range(3):
        in_copy(i).start()
    bar = pltpu.get_barrier_semaphore()
    pl.semaphore_signal(bar, inc=1, device_id=partner, device_id_type=MESH)
    for k in range(1, chips):
        pl.semaphore_signal(bar, inc=1, device_id=peer(chip(k)), device_id_type=MESH)
    for i in range(n_up):
        up_copy(i).start()
    for half in range(2):
        for i in range(chips):
            dn_copy(half, i).start()
    for i in range(slots):
        qkv_copy(i).start()
    for i in range(n_kv):
        kv_copy(0, i).start()
        kv_copy(1, i).start()
    pl.semaphore_wait(bar, chips)

    for i in range(3):
        in_copy(i).wait()

    @pl.loop(0, rows // 16)
    def _(i):
        sl = pl.ds(pl.multiple_of(i * 16, 16), 16)
        xf = x_s[sl, :].astype(F32)
        mean = jnp.mean(xf, axis=-1, keepdims=True)
        cen = xf - mean
        var = jnp.mean(cen * cen, axis=-1, keepdims=True)
        h_s[sl, :] = (cen * lax.rsqrt(var + LN_EPS) * gb_s[0:1, :] + gb_s[8:9, :]).astype(BF16)

    def chunk_dot(a_ref, row, depth):
        acc = None
        for kk in range(depth // BLK):
            w = w_s[pl.ds(pl.multiple_of(row + kk * BLK, BLK), BLK), :]
            p = jnp.dot(a_ref[:, kk * BLK:(kk + 1) * BLK], w, preferred_element_type=F32)
            acc = p if acc is None else acc + p
        return acc

    @pl.loop(0, n_up)
    def _(i):
        up_copy(i).wait()
        u = chunk_dot(h_s, i * up_rows, up_rows)
        g = 0.5 * u * (1.0 + lax.erf(u * (0.5 ** 0.5)))
        act_s[:, pl.ds(pl.multiple_of(i * BLK, BLK), BLK)] = g.astype(BF16)

    @pl.loop(0, chips)
    def _(i):
        dn_copy(0, i).wait()
        zz = order(i)
        ps_s[zz] = chunk_dot(act_s, dn_base + i * dn_rows, dn_rows)
        pd_copy(zz).start()

    @pl.loop(0, chips)
    def _(i):
        dn_copy(1, i).wait()
        zz = order(i)
        p = chunk_dot(act_s, dn_base + (chips + i) * dn_rows, dn_rows)
        pd_copy(zz).wait_recv()
        p = p + pr_s[zz]

        @pl.when(zz == z)
        def _():
            rs_s[z] = p

        @pl.when(zz != z)
        def _():
            ss_s[zz] = p
            rs_copy(zz, z).start()

    @pl.loop(0, slots)
    def _(i):
        qkv_copy(i).wait()
        a = chunk_dot(h_s, qkv_base + i * d_model, d_model).astype(BF16).astype(F32)
        a1, a2 = a[:, :HALF], a[:, HALF:]
        cs, sn = cos_ref[...], sin_ref[...]
        r1 = (a1 * cs - a2 * sn).astype(BF16).astype(F32)
        r2 = (a2 * cs + a1 * sn).astype(BF16).astype(F32)
        slot = c * slots + i
        is_v = slot == heads + 1
        row = pl.multiple_of(slot * 2 * rows, 8)
        qk_s[pl.ds(row, rows), :] = jnp.where(is_v, a1, r1)
        qk_s[pl.ds(row + rows, rows), :] = jnp.where(is_v, a2, r2)
        qx_copy(c, i).start()

    for i in range(n_col):
        wo_copy(i).start()

    for i in range(slots):
        qx_copy(pc, i).wait_recv()
    for t in range(2):
        sl = slice(t * HALF, (t + 1) * HALF)
        knew_ref[:, sl] = qk_s[(2 * heads + t) * rows:(2 * heads + t + 1) * rows, :].astype(BF16)
        vnew_ref[:, sl] = qk_s[(2 * heads + 2 + t) * rows:(2 * heads + 3 + t) * rows, :].astype(BF16)

    lane = lax.broadcasted_iota(jnp.int32, (heads, seq), 1)
    scale = k_s.shape[2] ** -0.5

    def attend(b, carry):
        mm, ll = carry
        def both(base, n):
            return jnp.concatenate([qk_s[pl.ds(base + b, n, stride=2 * rows), :], qk_s[pl.ds(base + rows + b, n, stride=2 * rows), :]], axis=-1)

        def one(base):
            return jnp.concatenate([qk_s[pl.ds(base + b, 1), :], qk_s[pl.ds(base + rows + b, 1), :]], axis=-1)

        q = both(0, heads)
        kn = one(2 * heads * rows)
        vn = one((2 * heads + 2) * rows)
        lp = lp_ref[pl.ds(b, 1), :]
        sc = lax.dot_general(q.astype(BF16), k_s[b], (((1,), (1,)), ((), ())), preferred_element_type=F32)
        here = lane == lp
        sc = jnp.where(here, jnp.sum(q * kn, axis=-1, keepdims=True), sc) * scale
        valid = lane <= lp
        sc = jnp.where(valid, sc, NEG_FILL)
        m = jnp.max(sc, axis=-1, keepdims=True)
        e = jnp.where(valid, jnp.exp(sc - m), 0.0)
        l = jnp.sum(e, axis=-1, keepdims=True)
        eb = e.astype(BF16).astype(F32)
        e_new = jnp.sum(jnp.where(here, eb, 0.0), axis=-1, keepdims=True)
        o = jnp.dot(jnp.where(here, 0.0, eb).astype(BF16), v_s[b], preferred_element_type=F32) + e_new * vn
        ost_s[0, pl.ds(pl.multiple_of(b * half_heads, 8), half_heads), :] = o[:half_heads]
        ost_s[1, pl.ds(pl.multiple_of(b * half_heads, 8), half_heads), :] = o[half_heads:]
        col = lane == b
        return jnp.where(col, m, mm), jnp.where(col, l, ll)

    zero = jnp.zeros((heads, seq), F32)
    carry = (zero, zero)
    for i in range(n_kv):
        kv_copy(0, i).wait()
        kv_copy(1, i).wait()
        carry = lax.fori_loop(i * kv_rows, (i + 1) * kv_rows, attend, carry, unroll=4)
    mm, ll = carry
    ml = jnp.concatenate([mm, ll], axis=-1)
    ost_s[0, rows * half_heads:, :] = ml[:half_heads]
    ost_s[1, rows * half_heads:, :] = ml[half_heads:]
    st_copy().start()

    for k in range(1, chips):
        rs_copy(chip(k), chip(k)).wait_recv()
    tot = rs_s[0]
    for j in range(1, chips):
        tot = tot + rs_s[j]
    ma_s[c * chips + z] = tot
    for k in range(1, chips):
        ma_copy(chip(k), z).start()
    ma_fwd(c, z).start()

    st_copy().wait_recv()
    base = rows * half_heads
    m_s, l_s = ost_s[c, base:, :HALF], ost_s[c, base:, HALF:]
    m_p, l_p = orx_s[base:, :HALF], orx_s[base:, HALF:]
    m_c = jnp.maximum(m_s, m_p)
    w_own, w_par = jnp.exp(m_s - m_c), jnp.exp(m_p - m_c)
    def put(b, lo, hi):
        cz_s[pl.ds(b, half_heads, stride=2 * tail), :] = lo
        cz_s[pl.ds(tail + b, half_heads, stride=2 * tail), :] = hi

    for b in range(rows):
        sl = slice(b * half_heads, (b + 1) * half_heads)
        mix = ost_s[c, sl, :] * w_own[:, b:b + 1] + orx_s[sl, :] * w_par[:, b:b + 1]
        put(b, mix[:, :HALF], mix[:, HALF:])
    put(rows, m_c, l_s * w_own + l_p * w_par)
    nil = jnp.zeros((half_heads, HALF), F32)
    for b in range(rows + 1, tail):
        put(b, nil, nil)
    for k in range(1, chips):
        aa_copy(chip(k), z).start()
    mine = pl.ds(pl.multiple_of(z * 2 * tail, 8), 2 * tail)
    r_s[mine, :] = cz_s[mine, :]

    for k in range(1, chips):
        aa_copy(chip(k), chip(k)).wait_recv()
    m_all = r_s[pl.ds(rows, chips, stride=2 * tail), :]
    l_all = r_s[pl.ds(tail + rows, chips, stride=2 * tail), :]
    w_all = jnp.exp(m_all - jnp.max(m_all, axis=0, keepdims=True))
    l_tot = jnp.sum(l_all * w_all, axis=0, keepdims=True)
    w_t = jnp.transpose(w_all)[:rows]
    l_t = jnp.transpose(jnp.broadcast_to(l_tot, w_all.shape))[:rows]
    for t in range(2):
        ctx = None
        for j in range(chips):
            at = (2 * j + t) * tail
            part = r_s[at:at + rows, :] * w_t[:, j:j + 1]
            ctx = part if ctx is None else ctx + part
        g_s[c * chips + z, :, t * HALF:(t + 1) * HALF] = (ctx / l_t[:, 0:1]).astype(BF16).astype(F32)
    for k in range(1, chips):
        cg_copy(chip(k), z).start()
    cg_fwd(c, z).start()

    for i in range(n_col):
        wo_copy(i).wait()

    def out_dot(slot, first=False):
        a = g_s[slot].astype(BF16)
        for n in range(n_col):
            w = w_s[pl.ds(pl.multiple_of(n * d_model + slot * BLK, BLK), BLK), :]
            p = jnp.dot(a, w, preferred_element_type=F32)
            sl = slice(n * BLK, (n + 1) * BLK)
            acc_s[:, sl] = p if first else acc_s[:, sl] + p

    out_dot(c * chips + z, True)
    for k in range(1, chips):
        ma_copy(chip(k), chip(k)).wait_recv()
        ma_fwd(c, chip(k)).start()

    @pl.loop(1, chips)
    def _(k):
        cg_copy(chip(k), chip(k)).wait_recv()
        cg_fwd(c, chip(k)).start()
        out_dot(c * chips + chip(k))

    @pl.loop(0, chips)
    def _(k):
        cg_fwd(pc, chip(k)).wait_recv()
        out_dot(pc * chips + chip(k))

    for k in range(chips):
        ma_fwd(pc, chip(k)).wait_recv()
    for n in range(n_col):
        sl = slice(n * BLK, (n + 1) * BLK)
        out_ref[:, sl] = (x_s[:, sl].astype(F32) + acc_s[:, sl] + ma_s[n]).astype(BF16)

    for k in range(chips):
        pd_copy(chip(k)).wait_send()
        ma_fwd(c, chip(k)).wait_send()
        cg_fwd(c, chip(k)).wait_send()
    for k in range(1, chips):
        rs_copy(chip(k), z).wait_send()
        ma_copy(chip(k), z).wait_send()
        aa_copy(chip(k), z).wait_send()
        cg_copy(chip(k), z).wait_send()
    for i in range(slots):
        qx_copy(c, i).wait_send()
    st_copy().wait_send()


def device_step(n_sp, hidden, ln_gamma, ln_beta, w_qkv, w_out, w_up, w_down, k_cache, v_cache, positions):
    rows, d_model = hidden.shape
    seq, head_dim = k_cache.shape[1], k_cache.shape[2]
    heads = w_out.shape[0] // head_dim
    ff = w_up.shape[1]
    chips = n_sp // 2
    slots = (heads + 2) // 2
    assert head_dim == BLK and heads == n_sp and d_model == n_sp * BLK
    cos, sin = rotary_tables(positions, head_dim)
    local_pos = positions - lax.axis_index('sp') * seq
    lp = jnp.broadcast_to(local_pos[:, None], (rows, seq))
    n_up, n_col = ff // BLK, d_model // BLK
    w_rows = n_up * d_model + n_col * ff + slots * d_model
    n_kv = 3
    half = heads // 2
    any_spec = pl.BlockSpec(memory_space=pl.ANY)
    vmem_spec = pl.BlockSpec(memory_space=pltpu.VMEM)
    dma = pltpu.SemaphoreType.DMA
    scratch = [
        pltpu.VMEM((rows, d_model), BF16),
        pltpu.VMEM((16, d_model), F32),
        pltpu.VMEM((rows, d_model), BF16),
        pltpu.VMEM((rows, ff), BF16),
        pltpu.VMEM((w_rows, BLK), BF16),
        pltpu.VMEM(k_cache.shape, BF16),
        pltpu.VMEM(v_cache.shape, BF16),
        pltpu.VMEM(((heads + 2) * 2 * rows, HALF), F32),
        pltpu.VMEM((chips, rows, BLK), F32),
        pltpu.VMEM((chips, rows, BLK), F32),
        pltpu.VMEM((chips, rows, BLK), F32),
        pltpu.VMEM((chips, rows, BLK), F32),
        pltpu.VMEM((n_sp, rows, BLK), F32),
        pltpu.VMEM((2, (rows + 1) * half, BLK), F32),
        pltpu.VMEM(((rows + 1) * half, BLK), F32),
        pltpu.VMEM((chips * 2 * (rows + 8), HALF), F32),
        pltpu.VMEM((chips * 2 * (rows + 8), HALF), F32),
        pltpu.VMEM((n_sp, rows, BLK), F32),
        pltpu.VMEM((rows, d_model), F32),
        dma((3,)), dma((n_up,)), dma((n_col,)), dma((slots,)), dma((2, n_kv)), dma((n_col,)),
        dma((chips,)), dma((chips,)), dma((chips,)), dma((chips,)), dma((chips,)), dma((chips,)), dma((n_sp,)),
        dma((slots,)), dma((slots,)), dma((1,)), dma((1,)), dma((chips,)), dma((chips,)), dma((chips,)), dma((chips,)), dma((n_sp,)),
    ]
    out, k_new, v_new = pl.pallas_call(
        functools.partial(layer_kernel, chips, heads),
        out_shape=(jax.ShapeDtypeStruct((rows, d_model), BF16), jax.ShapeDtypeStruct((rows, BLK), BF16), jax.ShapeDtypeStruct((rows, BLK), BF16)),
        in_specs=[any_spec] * 9 + [vmem_spec] * 3,
        out_specs=(vmem_spec, vmem_spec, vmem_spec),
        scratch_shapes=scratch,
        compiler_params=pltpu.CompilerParams(collective_id=0, has_side_effects=True, vmem_limit_bytes=63 * 1024 * 1024),
        name='decode_layer',
    )(hidden, ln_gamma.reshape(1, -1), ln_beta.reshape(1, -1), w_qkv, w_out, w_up, w_down, k_cache, v_cache, cos, sin, lp)
    write_mask = (jnp.arange(seq)[None, :] == local_pos[:, None])[:, :, None]
    k_next = jnp.where(write_mask, k_new[:, None, :], k_cache)
    v_next = jnp.where(write_mask, v_new[:, None, :], v_cache)
    return out, k_next, v_next


def solution(mesh):
    cache_spec = P('dp', 'sp', None)
    in_specs = (P('dp', None), P(None), P(None), P(None, None), P(None, None), P(None, 'sp'), P('sp', None), cache_spec, cache_spec, P('dp'))
    out_specs = (P('dp', None), cache_spec, cache_spec)
    return jax.shard_map(functools.partial(device_step, mesh.shape['sp']), mesh=mesh, in_specs=in_specs, out_specs=out_specs, check_vma=False)
```

```python
import functools

import jax
import jax.numpy as jnp
from jax import lax
from jax.experimental import pallas as pl
from jax.experimental.pallas import tpu as pltpu
from jax.sharding import PartitionSpec as P

LN_EPS = 1e-5
ROPE_BASE = 10000.0
NEG_FILL = -1e30
MESH = pl.DeviceIdType.MESH
BLK = 256
HALF = 128
F32 = jnp.float32
BF16 = jnp.bfloat16


ORDER = (3, -3, 4, 2, -2, 1, -1, 0)


class Phases:
    def __init__(self):
        self.scope = None

    def __call__(self, name):
        if self.scope is not None:
            self.scope.__exit__(None, None, None)
        self.scope = jax.named_scope(name) if name else None
        if self.scope is not None:
            self.scope.__enter__()


def layer_kernel(chips, heads, x_hbm, gamma_hbm, beta_hbm, wqkv_hbm, wout_hbm, wup_hbm, wdown_hbm, k_hbm, v_hbm, pos_hbm,
                 inv_ref, out_ref, knew_ref, vnew_ref,
                 x_s, gb_s, h_s, act_s, w_s, k_s, v_s, pos_s, lp_s, cs_s, sn_s, qk_s,
                 ps_s, pr_s, ss_s, ra_s, rb_s, ma_s, ost_s, orx_s, cz_s, ta_s, tb_s, tw_s, g_s, acc_s,
                 in_sem, up_sem, dn_sem, qkv_sem, kv_sem, wo_sem,
                 pd_send, pd_recv, qx_send, qx_recv, st_send, st_recv,
                 rs_send, rs_recv, aa_send, aa_recv, ma_send, ma_recv, mf_send, mf_recv, cg_send, cg_recv, cf_send, cf_recv):
    rows, d_model = x_hbm.shape
    ff = wup_hbm.shape[1]
    seq = k_hbm.shape[1]
    n_up = ff // BLK
    n_col = d_model // BLK
    half_heads = heads // 2
    slots = (heads + 2) // 2
    hr = rows // 2
    ml_at = 2 * hr
    hi_at = ml_at + 8
    chunk = 4 * hr + 8
    part = 2 * hr + 8
    up_rows, dn_rows = d_model, ff
    dn_base = n_up * up_rows
    qkv_base = dn_base + n_col * dn_rows
    n_kv = kv_sem.shape[1]
    kv_rows = rows // n_kv

    s = lax.axis_index('sp')
    z = lax.div(s, 2)
    c = lax.rem(s, 2)
    pc = 1 - c
    partner = {'sp': 2 * z + pc}

    def chip(k):
        return lax.rem(z + (k % chips), chips)

    def peer(k):
        return {'sp': 2 * chip(k) + c}

    def in_copy(i):
        src, dst = ((x_hbm, x_s), (gamma_hbm, gb_s.at[pl.ds(0, 1)]), (beta_hbm, gb_s.at[pl.ds(8, 1)]), (pos_hbm, pos_s))[i]
        return pltpu.make_async_copy(src, dst, in_sem.at[i])

    def up_copy(i):
        col = pl.multiple_of(i * BLK, BLK)
        row = pl.multiple_of(i * up_rows, BLK)
        return pltpu.make_async_copy(wup_hbm.at[:, pl.ds(col, BLK)], w_s.at[pl.ds(row, up_rows)], up_sem.at[i])

    def dn_copy(half, i):
        owner = pc if half == 0 else c
        col = pl.multiple_of((owner * chips + chip(ORDER[i])) * BLK, BLK)
        slot = half * chips + i
        row = pl.multiple_of(dn_base + slot * dn_rows, BLK)
        return pltpu.make_async_copy(wdown_hbm.at[:, pl.ds(col, BLK)], w_s.at[pl.ds(row, dn_rows)], dn_sem.at[slot])

    def qkv_copy(i):
        col = pl.multiple_of((c * slots + i) * BLK, BLK)
        row = pl.multiple_of(qkv_base + i * d_model, BLK)
        return pltpu.make_async_copy(wqkv_hbm.at[:, pl.ds(col, BLK)], w_s.at[pl.ds(row, d_model)], qkv_sem.at[i])

    def kv_copy(t, i):
        src, dst = ((k_hbm, k_s), (v_hbm, v_s))[t]
        sl = pl.ds(i * kv_rows, kv_rows)
        return pltpu.make_async_copy(src.at[sl], dst.at[sl], kv_sem.at[t, i])

    def wo_copy(i):
        col = pl.multiple_of(i * BLK, BLK)
        row = pl.multiple_of(i * d_model, BLK)
        return pltpu.make_async_copy(wout_hbm.at[:, pl.ds(col, BLK)], w_s.at[pl.ds(row, d_model)], wo_sem.at[i])

    def remote(src, dst, send, recv, to):
        return pltpu.make_async_remote_copy(src, dst, send, recv, device_id=to, device_id_type=MESH)

    def pd_copy(i):
        return remote(ps_s.at[i], pr_s.at[i], pd_send.at[i], pd_recv.at[i], partner)

    def qx_copy(owner, i):
        row = pl.multiple_of((owner * slots + i) * 2 * rows, 8)
        ref = qk_s.at[pl.ds(row, 2 * rows)]
        return remote(ref, ref, qx_send.at[i], qx_recv.at[i], partner)

    def st_copy():
        return remote(ost_s.at[pc], orx_s, st_send.at[0], st_recv.at[0], partner)

    hops = (1, -1, 2, -2, 2, -2, 1, -1)

    def rs_copy(i):
        src = (ss_s.at[0], ss_s.at[1], ss_s.at[2, pl.ds(0, hr)], ss_s.at[2, pl.ds(hr, hr)], ss_s.at[3], ss_s.at[4], ss_s.at[5], ss_s.at[6])[i]
        dst = (ra_s.at[0], ra_s.at[1], ra_s.at[2, pl.ds(0, hr)], ra_s.at[2, pl.ds(hr, hr)], rb_s.at[0], rb_s.at[1], rb_s.at[2], rb_s.at[3])[i]
        return remote(src, dst, rs_send.at[i], rs_recv.at[i], peer(hops[i]))

    def cz_at(k, off, n):
        return cz_s.at[pl.ds(pl.multiple_of(chip(k) * chunk + off, 8), n)]

    def aa_copy(i):
        src = (lambda: cz_at(3, 0, chunk), lambda: cz_at(-3, 0, chunk), lambda: cz_at(4, 0, part), lambda: cz_at(4, ml_at, part),
               lambda: tw_s.at[0], lambda: tw_s.at[1], lambda: cz_at(1, 0, chunk), lambda: cz_at(-1, 0, chunk))[i]()
        dst = (ta_s.at[0], ta_s.at[1], ta_s.at[2, pl.ds(0, part)], ta_s.at[3, pl.ds(0, part)], tb_s.at[0], tb_s.at[1], tb_s.at[2], tb_s.at[3])[i]
        return remote(src, dst, aa_send.at[i], aa_recv.at[i], peer(hops[i]))

    g_hop = (2, -2, 1, -1, 1, -1, 2, -2)
    g_src = (0, 0, 0, 0, -2, 2, -2, 2)

    def gather_copy(buf, send, recv, i):
        ref = buf.at[c * chips + chip(g_src[i])]
        if i >= 6:
            ref = ref.at[pl.ds((i - 6) * hr, hr)]
        return remote(ref, ref, send.at[i], recv.at[i], peer(g_hop[i]))

    def gather_recv(buf, send, recv, i):
        ref = buf.at[c * chips + chip(g_src[i] - g_hop[i])]
        if i >= 6:
            ref = ref.at[pl.ds((i - 6) * hr, hr)]
        return remote(ref, ref, send.at[i], recv.at[i], peer(g_hop[i]))

    def ma_copy(i):
        return gather_copy(ma_s, ma_send, ma_recv, i)

    def cg_copy(i):
        return gather_copy(g_s, cg_send, cg_recv, i)

    def ma_wait(i):
        gather_recv(ma_s, ma_send, ma_recv, i).wait_recv()

    def cg_wait(i):
        gather_recv(g_s, cg_send, cg_recv, i).wait_recv()

    def ma_fwd(owner, k):
        ref = ma_s.at[owner * chips + chip(k)]
        return remote(ref, ref, mf_send.at[k % chips], mf_recv.at[k % chips], partner)

    def cg_fwd(owner, k):
        ref = g_s.at[owner * chips + chip(k)]
        return remote(ref, ref, cf_send.at[k % chips], cf_recv.at[k % chips], partner)

    ph = Phases()
    ph('entry')
    for i in range(4):
        in_copy(i).start()
    for i in range(n_up):
        up_copy(i).start()
    bar = pltpu.get_barrier_semaphore()
    pl.semaphore_signal(bar, inc=1, device_id=partner, device_id_type=MESH)
    for k in (1, -1, 2, -2):
        pl.semaphore_signal(bar, inc=1, device_id=peer(k), device_id_type=MESH)
    for half in range(2):
        for i in range(chips):
            dn_copy(half, i).start()
    for i in range(slots):
        qkv_copy(i).start()
    for i in range(n_kv):
        kv_copy(0, i).start()
        kv_copy(1, i).start()

    ph('in_wait')
    for i in range(4):
        in_copy(i).wait()
    ph('layer_norm')

    @pl.loop(0, rows // 16)
    def _(i):
        sl = pl.ds(pl.multiple_of(i * 16, 16), 16)
        xf = x_s[sl, :].astype(F32)
        mean = jnp.mean(xf, axis=-1, keepdims=True)
        cen = xf - mean
        var = jnp.mean(cen * cen, axis=-1, keepdims=True)
        h_s[sl, :] = (cen * lax.rsqrt(var + LN_EPS) * gb_s[0:1, :] + gb_s[8:9, :]).astype(BF16)

    ph('rope')
    for b in range(rows):
        lp_s[b:b + 1, :] = jnp.full((1, HALF), pos_s[b], jnp.int32).astype(F32)
    ang = lp_s[...] * inv_ref[...]
    cs_s[...] = jnp.cos(ang)
    sn_s[...] = jnp.sin(ang)
    lp_s[...] = lp_s[...] - (s * seq).astype(F32)

    def chunk_dots(a_ref, bases, depth):
        accs = [None] * len(bases)
        for kk in range(depth // BLK):
            a = a_ref[:, kk * BLK:(kk + 1) * BLK]
            for j, row in enumerate(bases):
                w = w_s[pl.ds(pl.multiple_of(row + kk * BLK, BLK), BLK), :]
                p = jnp.dot(a, w, preferred_element_type=F32)
                accs[j] = p if accs[j] is None else accs[j] + p
        return accs

    ph('mlp_up')

    @pl.loop(0, n_up // 2)
    def _(i):
        up_copy(2 * i).wait()
        up_copy(2 * i + 1).wait()
        us = chunk_dots(h_s, [(2 * i + j) * up_rows for j in range(2)], up_rows)
        for j, u in enumerate(us):
            g = 0.5 * u * (1.0 + lax.erf(u * (0.5 ** 0.5)))
            act_s[:, pl.ds(pl.multiple_of((2 * i + j) * BLK, BLK), BLK)] = g.astype(BF16)

    ph('barrier')
    pl.semaphore_wait(bar, 5)
    ph('down_partner')
    for i in range(0, chips, 2):
        for j in range(2):
            dn_copy(0, i + j).wait()
        for j, p in enumerate(chunk_dots(act_s, [dn_base + (i + j) * dn_rows for j in range(2)], dn_rows)):
            ps_s[i + j] = p
            pd_copy(i + j).start()

    ph('down_own')
    for i in range(0, chips, 2):
        for j in range(2):
            dn_copy(1, i + j).wait()
        for j, p in enumerate(chunk_dots(act_s, [dn_base + (chips + i + j) * dn_rows for j in range(2)], dn_rows)):
            n = i + j
            pd_copy(n).wait_recv()
            ss_s[n] = p + pr_s[n]
            for m in ((0,), (1,), (2, 3), (), (), (6,), (7,), ())[n]:
                rs_copy(m).start()

    def qkv_store(i, acc):
        a = acc.astype(BF16).astype(F32)
        a1, a2 = a[:, :HALF], a[:, HALF:]
        cs, sn = cs_s[...], sn_s[...]
        r1 = (a1 * cs - a2 * sn).astype(BF16).astype(F32)
        r2 = (a2 * cs + a1 * sn).astype(BF16).astype(F32)
        slot = c * slots + i
        is_v = slot == heads + 1
        row = pl.multiple_of(slot * 2 * rows, 8)
        qk_s[pl.ds(row, rows), :] = jnp.where(is_v, a1, r1)
        qk_s[pl.ds(row + rows, rows), :] = jnp.where(is_v, a2, r2)
        qx_copy(c, i).start()

    def qkv_pair(i):
        qkv_copy(2 * i).wait()
        qkv_copy(2 * i + 1).wait()
        for j, acc in enumerate(chunk_dots(h_s, [qkv_base + (2 * i + j) * d_model for j in range(2)], d_model)):
            qkv_store(2 * i + j, acc)

    n_pair = slots // 2
    ph('qkv')
    pl.loop(0, n_pair - 1)(qkv_pair)

    ph('rs_add')
    for i in range(4):
        rs_copy(i).wait_recv()
    ss_s[3, 0:hr] = ss_s[3, 0:hr] + ra_s[0, 0:hr] + ra_s[2, 0:hr]
    ss_s[3, hr:] = ss_s[3, hr:] + ra_s[0, hr:]
    ss_s[4, 0:hr] = ss_s[4, 0:hr] + ra_s[1, 0:hr]
    ss_s[4, hr:] = ss_s[4, hr:] + ra_s[1, hr:] + ra_s[2, hr:]
    rs_copy(4).start()
    rs_copy(5).start()
    ph('qkv_last')
    qkv_pair(n_pair - 1)
    for i in range(2 * n_pair, slots):
        qkv_copy(i).wait()
        qkv_store(i, chunk_dots(h_s, [qkv_base + i * d_model], d_model)[0])

    for i in range(n_col):
        wo_copy(i).start()

    ph('qkv_wait')
    for i in range(slots):
        qx_copy(pc, i).wait_recv()
    for t in range(2):
        sl = slice(t * HALF, (t + 1) * HALF)
        knew_ref[:, sl] = qk_s[(2 * heads + t) * rows:(2 * heads + t + 1) * rows, :].astype(BF16)
        vnew_ref[:, sl] = qk_s[(2 * heads + 2 + t) * rows:(2 * heads + 3 + t) * rows, :].astype(BF16)

    lane = lax.broadcasted_iota(jnp.int32, (heads, seq), 1)
    lane_f = lane.astype(F32)
    scale = k_s.shape[2] ** -0.5
    group = rows // 4

    def attend(g, carry):
        mm, ll = carry
        base = g * group
        scores, values, here = [], [], []
        for r in range(group):
            b = base + r

            def both(at, n):
                return jnp.concatenate([qk_s[pl.ds(at + b, n, stride=2 * rows), :], qk_s[pl.ds(at + rows + b, n, stride=2 * rows), :]], axis=-1)

            def one(at):
                return jnp.concatenate([qk_s[pl.ds(at + b, 1), :], qk_s[pl.ds(at + rows + b, 1), :]], axis=-1)

            q = both(0, heads)
            kn = one(2 * heads * rows)
            lp = lp_s[pl.ds(b, 1), :]
            here.append(lane_f == lp)
            sc = lax.dot_general(q.astype(BF16), k_s[b], (((1,), (1,)), ((), ())), preferred_element_type=F32)
            sc = jnp.where(here[r], jnp.sum(q * kn, axis=-1, keepdims=True), sc) * scale
            scores.append(jnp.where(lane_f <= lp, sc, NEG_FILL))
            values.append(one((2 * heads + 2) * rows))
        es, news = [], []
        for r in range(group):
            m = jnp.max(scores[r], axis=-1, keepdims=True)
            e = jnp.where(lane_f <= lp_s[pl.ds(base + r, 1), :], jnp.exp(scores[r] - m), 0.0)
            col = lane == base + r
            mm = jnp.where(col, m, mm)
            ll = jnp.where(col, jnp.sum(e, axis=-1, keepdims=True), ll)
            eb = e.astype(BF16).astype(F32)
            news.append(jnp.sum(jnp.where(here[r], eb, 0.0), axis=-1, keepdims=True))
            es.append(jnp.where(here[r], 0.0, eb).astype(BF16))
        for r in range(group):
            b = base + r
            o = jnp.dot(es[r], v_s[b], preferred_element_type=F32) + news[r] * values[r]
            at = pl.ds(pl.multiple_of(b * half_heads, 8), half_heads)
            ost_s[0, at, :] = o[:half_heads]
            ost_s[1, at, :] = o[half_heads:]
        return mm, ll

    ph('kv_wait')
    for i in range(n_kv):
        kv_copy(0, i).wait()
        kv_copy(1, i).wait()
    ph('attention')
    zero = jnp.zeros((heads, seq), F32)
    mm, ll = lax.fori_loop(0, 3, attend, (zero, zero))

    ph('rs_sum')
    for i in range(4, 8):
        rs_copy(i).wait_recv()
    ma_s[c * chips + z] = ss_s[7] + rb_s[0] + rb_s[1] + rb_s[2] + rb_s[3]
    for i in range(4):
        ma_copy(i).start()
    ma_fwd(c, 0).start()

    ph('attention_last')
    mm, ll = lax.fori_loop(3, 4, attend, (mm, ll))
    ml = jnp.concatenate([mm, ll], axis=-1)
    ost_s[0, rows * half_heads:, :] = ml[:half_heads]
    ost_s[1, rows * half_heads:, :] = ml[half_heads:]
    st_copy().start()

    ph('stat_wait')
    st_copy().wait_recv()
    ph('merge')
    base = rows * half_heads
    m_s, l_s = ost_s[c, base:, :HALF], ost_s[c, base:, HALF:]
    m_p, l_p = orx_s[base:, :HALF], orx_s[base:, HALF:]
    m_c = jnp.maximum(m_s, m_p)
    w_own, w_par = jnp.exp(m_s - m_c), jnp.exp(m_p - m_c)

    def put(at, val):
        cz_s[pl.ds(at, half_heads, stride=chunk), :] = val

    for b in range(rows):
        sl = slice(b * half_heads, (b + 1) * half_heads)
        mix = ost_s[c, sl, :] * w_own[:, b:b + 1] + orx_s[sl, :] * w_par[:, b:b + 1]
        at = b if b < hr else hi_at + b - hr
        put(at, mix[:, :HALF])
        put(at + hr, mix[:, HALF:])
    put(ml_at, m_c)
    put(ml_at + 1, l_s * w_own + l_p * w_par)
    nil = jnp.zeros((half_heads, HALF), F32)
    for i in range(2, 8):
        put(ml_at + i, nil)
    for i in (0, 1, 2, 3, 6, 7):
        aa_copy(i).start()

    row_lane = lax.broadcasted_iota(jnp.int32, (1, HALF), 1)
    is_lo = row_lane < hr

    def blend(parts, out):
        ms, ls = [], []
        for ref, at, lo, hi in parts:
            m, l = ref[at:at + 1, :], ref[at + 1:at + 2, :]
            if lo is None:
                m, l = jnp.where(is_lo, NEG_FILL, m), jnp.where(is_lo, 0.0, l)
            if hi is None:
                m, l = jnp.where(is_lo, m, NEG_FILL), jnp.where(is_lo, l, 0.0)
            ms.append(m)
            ls.append(l)
        top = functools.reduce(jnp.maximum, ms)
        ws = [jnp.exp(m - top) for m in ms]
        l_sum = functools.reduce(lambda a, b: a + b, [l * w for l, w in zip(ls, ws)])
        pad = [jnp.zeros_like(top)] * (8 - len(parts) - 1)
        cols = jnp.transpose(jnp.concatenate(ws + [l_sum] + pad, axis=0))
        for half in range(2):
            for t in range(2):
                acc = None
                for j, (ref, at, lo, hi) in enumerate(parts):
                    off = (lo, hi)[half]
                    if off is None:
                        continue
                    term = ref[off + t * hr:off + (t + 1) * hr, :] * cols[half * hr:(half + 1) * hr, j:j + 1]
                    acc = term if acc is None else acc + term
                out(half, t, acc, cols[half * hr:(half + 1) * hr, len(parts):len(parts) + 1])
        return top, l_sum

    ph('aa_wait')
    for i in range(4):
        aa_copy(i).wait_recv()
    ph('aa_add')
    for side, k in ((0, 2), (1, -2)):
        half_part = (ta_s.at[2], ml_at, 0, None) if side == 0 else (ta_s.at[3], 0, None, 8)

        def keep(half, t, acc, _, side=side):
            off = (0, hi_at)[half] + t * hr
            tw_s[side, off:off + hr, :] = acc

        top, l_sum = blend([(cz_at(k, 0, chunk), ml_at, 0, hi_at), (ta_s.at[side], ml_at, 0, hi_at), half_part], keep)
        tw_s[side, ml_at:ml_at + 8, :] = jnp.concatenate([top, l_sum, jnp.zeros((6, HALF), F32)], axis=0)
        aa_copy(4 + side).start()

    ph('ma_on')
    ma_wait(0)
    ma_wait(1)
    for i in range(4, 8):
        ma_copy(i).start()
    ma_wait(2)
    ma_wait(3)
    for k in (2, -2, 1, -1):
        ma_fwd(c, k).start()

    ph('aa_wait2')
    for i in range(4, 8):
        aa_copy(i).wait_recv()
    ph('context')

    def finish(half, t, acc, l_col):
        g_s[c * chips + z, half * hr:(half + 1) * hr, t * HALF:(t + 1) * HALF] = (acc / l_col).astype(BF16).astype(F32)

    blend([(cz_at(0, 0, chunk), ml_at, 0, hi_at)] + [(tb_s.at[j], ml_at, 0, hi_at) for j in range(4)], finish)
    for i in range(4):
        cg_copy(i).start()
    cg_fwd(c, 0).start()

    ph('wo_wait')
    for i in range(n_col):
        wo_copy(i).wait()

    def out_dots(todo, first=False):
        lhs = [g_s[slot].astype(BF16) for slot in todo]
        for n in range(n_col):
            acc = None
            for slot, a in zip(todo, lhs):
                w = w_s[pl.ds(pl.multiple_of(n * d_model + slot * BLK, BLK), BLK), :]
                p = jnp.dot(a, w, preferred_element_type=F32)
                acc = p if acc is None else acc + p
            sl = slice(n * BLK, (n + 1) * BLK)
            acc_s[:, sl] = acc if first else acc_s[:, sl] + acc

    def mine(k):
        return c * chips + chip(k)

    def theirs(k):
        return pc * chips + chip(k)

    ph('out_0')
    out_dots([mine(0)], True)
    ph('ma_tail')
    for i in range(4, 8):
        ma_wait(i)
    for k in (3, -3, 4):
        ma_fwd(c, k).start()
    ph('cg_wait0')
    cg_fwd(pc, 0).wait_recv()
    cg_wait(0)
    cg_copy(4).start()
    cg_copy(6).start()
    cg_fwd(c, -2).start()
    cg_wait(1)
    cg_copy(5).start()
    cg_copy(7).start()
    cg_fwd(c, 2).start()
    ph('out_1')
    out_dots([theirs(0), mine(-2), mine(2)])
    ph('cg_wait1')
    cg_wait(2)
    cg_fwd(c, -1).start()
    cg_wait(3)
    cg_fwd(c, 1).start()
    ph('out_2')
    out_dots([mine(-1), mine(1)])
    ph('cg_wait2')
    cg_fwd(pc, -2).wait_recv()
    cg_fwd(pc, 2).wait_recv()
    ph('out_3')
    out_dots([theirs(-2), theirs(2)])
    ph('cg_wait3')
    cg_wait(4)
    cg_fwd(c, -3).start()
    cg_wait(5)
    cg_fwd(c, 3).start()
    cg_fwd(pc, -1).wait_recv()
    cg_fwd(pc, 1).wait_recv()
    ph('out_4')
    out_dots([mine(-3), mine(3), theirs(-1), theirs(1)])
    ph('cg_wait4')
    cg_wait(6)
    cg_wait(7)
    cg_fwd(c, 4).start()
    ph('out_5')
    out_dots([mine(4)])
    ph('cg_wait5')
    cg_fwd(pc, -3).wait_recv()
    cg_fwd(pc, 3).wait_recv()
    cg_fwd(pc, 4).wait_recv()
    ph('out_6')
    out_dots([theirs(-3), theirs(3), theirs(4)])
    ph('final')
    for k in range(chips):
        ma_fwd(pc, k).wait_recv()
    for n in range(n_col):
        sl = slice(n * BLK, (n + 1) * BLK)
        out_ref[:, sl] = (x_s[:, sl].astype(F32) + acc_s[:, sl] + ma_s[n]).astype(BF16)

    ph('drain')
    for i in range(chips):
        pd_copy(i).wait_send()
        ma_fwd(c, i).wait_send()
        cg_fwd(c, i).wait_send()
    for i in range(8):
        rs_copy(i).wait_send()
        aa_copy(i).wait_send()
        ma_copy(i).wait_send()
        cg_copy(i).wait_send()
    for i in range(slots):
        qx_copy(c, i).wait_send()
    st_copy().wait_send()
    ph(None)


def device_step(n_sp, hidden, ln_gamma, ln_beta, w_qkv, w_out, w_up, w_down, k_cache, v_cache, positions):
    rows, d_model = hidden.shape
    seq, head_dim = k_cache.shape[1], k_cache.shape[2]
    heads = w_out.shape[0] // head_dim
    ff = w_up.shape[1]
    chips = n_sp // 2
    slots = (heads + 2) // 2
    assert head_dim == BLK and heads == n_sp and d_model == n_sp * BLK and chips == 8
    inv_freq = 1.0 / (ROPE_BASE ** (jnp.arange(0, head_dim, 2, dtype=F32) / head_dim))
    local_pos = positions - lax.axis_index('sp') * seq
    n_up, n_col = ff // BLK, d_model // BLK
    w_rows = n_up * d_model + n_col * ff + slots * d_model
    n_kv = 3
    half = heads // 2
    any_spec = pl.BlockSpec(memory_space=pl.ANY)
    vmem_spec = pl.BlockSpec(memory_space=pltpu.VMEM)
    dma = pltpu.SemaphoreType.DMA
    hr = rows // 2
    chunk, part = 4 * hr + 8, 2 * hr + 8
    scratch = [
        pltpu.VMEM((rows, d_model), BF16),
        pltpu.VMEM((16, d_model), F32),
        pltpu.VMEM((rows, d_model), BF16),
        pltpu.VMEM((rows, ff), BF16),
        pltpu.VMEM((w_rows, BLK), BF16),
        pltpu.VMEM(k_cache.shape, BF16),
        pltpu.VMEM(v_cache.shape, BF16),
        pltpu.SMEM((rows,), jnp.int32),
        pltpu.VMEM((rows, HALF), F32),
        pltpu.VMEM((rows, HALF), F32),
        pltpu.VMEM((rows, HALF), F32),
        pltpu.VMEM(((heads + 2) * 2 * rows, HALF), F32),
        pltpu.VMEM((chips, rows, BLK), F32),
        pltpu.VMEM((chips, rows, BLK), F32),
        pltpu.VMEM((chips, rows, BLK), F32),
        pltpu.VMEM((3, rows, BLK), F32),
        pltpu.VMEM((4, rows, BLK), F32),
        pltpu.VMEM((n_sp, rows, BLK), F32),
        pltpu.VMEM((2, (rows + 1) * half, BLK), F32),
        pltpu.VMEM(((rows + 1) * half, BLK), F32),
        pltpu.VMEM((chips * chunk, HALF), F32),
        pltpu.VMEM((4, chunk, HALF), F32),
        pltpu.VMEM((4, chunk, HALF), F32),
        pltpu.VMEM((2, chunk, HALF), F32),
        pltpu.VMEM((n_sp, rows, BLK), F32),
        pltpu.VMEM((rows, d_model), F32),
        dma((4,)), dma((n_up,)), dma((n_col,)), dma((slots,)), dma((2, n_kv)), dma((n_col,)),
        dma((chips,)), dma((chips,)), dma((slots,)), dma((slots,)), dma((1,)), dma((1,)),
    ] + [dma((8,))] * 12
    out, k_new, v_new = pl.pallas_call(
        functools.partial(layer_kernel, chips, heads),
        out_shape=(jax.ShapeDtypeStruct((rows, d_model), BF16), jax.ShapeDtypeStruct((rows, BLK), BF16), jax.ShapeDtypeStruct((rows, BLK), BF16)),
        in_specs=[any_spec] * 10 + [vmem_spec],
        out_specs=(vmem_spec, vmem_spec, vmem_spec),
        scratch_shapes=scratch,
        compiler_params=pltpu.CompilerParams(collective_id=0, has_side_effects=True, vmem_limit_bytes=63 * 1024 * 1024),
        name='decode_layer',
    )(hidden, ln_gamma.reshape(1, -1), ln_beta.reshape(1, -1), w_qkv, w_out, w_up, w_down, k_cache, v_cache, positions, inv_freq.reshape(1, -1))
    write_mask = (jnp.arange(seq)[None, :] == local_pos[:, None])[:, :, None]
    k_next = jnp.where(write_mask, k_new[:, None, :], k_cache)
    v_next = jnp.where(write_mask, v_new[:, None, :], v_cache)
    return out, k_next, v_next


def solution(mesh):
    cache_spec = P('dp', 'sp', None)
    in_specs = (P('dp', None), P(None), P(None), P(None, None), P(None, None), P(None, 'sp'), P('sp', None), cache_spec, cache_spec, P('dp'))
    out_specs = (P('dp', None), cache_spec, cache_spec)
    return jax.shard_map(functools.partial(device_step, mesh.shape['sp']), mesh=mesh, in_specs=in_specs, out_specs=out_specs, check_vma=False)
```

```python
import functools

import jax
import jax.numpy as jnp
from jax import lax
from jax.experimental import pallas as pl
from jax.experimental.pallas import tpu as pltpu
from jax.sharding import PartitionSpec as P

LN_EPS = 1e-5
ROPE_BASE = 10000.0
NEG_FILL = -1e30
MESH = pl.DeviceIdType.MESH
BLK = 256
HALF = 128
F32 = jnp.float32
BF16 = jnp.bfloat16


ORDER = (3, -3, 4, 2, -2, 1, -1, 0)


class Phases:
    def __init__(self):
        self.scope = None

    def __call__(self, name):
        if self.scope is not None:
            self.scope.__exit__(None, None, None)
        self.scope = jax.named_scope(name) if name else None
        if self.scope is not None:
            self.scope.__enter__()


def layer_kernel(chips, heads, x_hbm, gamma_hbm, beta_hbm, wqkv_hbm, wout_hbm, wup_hbm, wdown_hbm, k_hbm, v_hbm, pos_hbm,
                 inv_ref, out_ref, k_s, v_s,
                 x_s, gb_s, h_s, act_s, w_s, pos_s, lp_s, cs_s, sn_s, qk_s,
                 ps_s, pr_s, ss_s, ra_s, rb_s, ma_s, ost_s, orx_s, cz_s, ta_s, tb_s, tw_s, g_s, acc_s,
                 in_sem, up_sem, dn_sem, qkv_sem, kv_sem, wo_sem,
                 pd_send, pd_recv, qx_send, qx_recv, st_send, st_recv,
                 rs_send, rs_recv, aa_send, aa_recv, ma_send, ma_recv, mf_send, mf_recv, cg_send, cg_recv, cf_send, cf_recv):
    rows, d_model = x_hbm.shape
    ff = wup_hbm.shape[1]
    seq = k_hbm.shape[1]
    n_up = ff // BLK
    n_col = d_model // BLK
    half_heads = heads // 2
    slots = (heads + 2) // 2
    hr = rows // 2
    ml_at = 2 * hr
    hi_at = ml_at + 8
    chunk = 4 * hr + 8
    part = 2 * hr + 8
    up_rows, dn_rows = d_model, ff
    dn_base = n_up * up_rows
    qkv_base = dn_base + n_col * dn_rows
    n_kv = kv_sem.shape[1]
    kv_rows = rows // n_kv

    s = lax.axis_index('sp')
    z = lax.div(s, 2)
    c = lax.rem(s, 2)
    pc = 1 - c
    partner = {'sp': 2 * z + pc}

    def chip(k):
        return lax.rem(z + (k % chips), chips)

    def peer(k):
        return {'sp': 2 * chip(k) + c}

    def in_copy(i):
        src, dst = ((x_hbm, x_s), (gamma_hbm, gb_s.at[pl.ds(0, 1)]), (beta_hbm, gb_s.at[pl.ds(8, 1)]), (pos_hbm, pos_s))[i]
        return pltpu.make_async_copy(src, dst, in_sem.at[i])

    def up_copy(i):
        col = pl.multiple_of(i * BLK, BLK)
        row = pl.multiple_of(i * up_rows, BLK)
        return pltpu.make_async_copy(wup_hbm.at[:, pl.ds(col, BLK)], w_s.at[pl.ds(row, up_rows)], up_sem.at[i])

    def dn_copy(half, i):
        owner = pc if half == 0 else c
        col = pl.multiple_of((owner * chips + chip(ORDER[i])) * BLK, BLK)
        slot = half * chips + i
        row = pl.multiple_of(dn_base + slot * dn_rows, BLK)
        return pltpu.make_async_copy(wdown_hbm.at[:, pl.ds(col, BLK)], w_s.at[pl.ds(row, dn_rows)], dn_sem.at[slot])

    def qkv_copy(i):
        col = pl.multiple_of((c * slots + i) * BLK, BLK)
        row = pl.multiple_of(qkv_base + i * d_model, BLK)
        return pltpu.make_async_copy(wqkv_hbm.at[:, pl.ds(col, BLK)], w_s.at[pl.ds(row, d_model)], qkv_sem.at[i])

    def kv_copy(t, i):
        src, dst = ((k_hbm, k_s), (v_hbm, v_s))[t]
        sl = pl.ds(i * kv_rows, kv_rows)
        return pltpu.make_async_copy(src.at[sl], dst.at[sl], kv_sem.at[t, i])

    def wo_copy(i):
        col = pl.multiple_of(i * BLK, BLK)
        row = pl.multiple_of(i * d_model, BLK)
        return pltpu.make_async_copy(wout_hbm.at[:, pl.ds(col, BLK)], w_s.at[pl.ds(row, d_model)], wo_sem.at[i])

    def remote(src, dst, send, recv, to):
        return pltpu.make_async_remote_copy(src, dst, send, recv, device_id=to, device_id_type=MESH)

    def pd_copy(i):
        return remote(ps_s.at[i], pr_s.at[i], pd_send.at[i], pd_recv.at[i], partner)

    def qx_copy(owner, i):
        row = pl.multiple_of((owner * slots + i) * 2 * rows, 8)
        ref = qk_s.at[pl.ds(row, 2 * rows)]
        return remote(ref, ref, qx_send.at[i], qx_recv.at[i], partner)

    def st_copy():
        return remote(ost_s.at[pc], orx_s, st_send.at[0], st_recv.at[0], partner)

    hops = (1, -1, 2, -2, 2, -2, 1, -1)

    def rs_copy(i):
        src = (ss_s.at[0], ss_s.at[1], ss_s.at[2, pl.ds(0, hr)], ss_s.at[2, pl.ds(hr, hr)], ss_s.at[3], ss_s.at[4], ss_s.at[5], ss_s.at[6])[i]
        dst = (ra_s.at[0], ra_s.at[1], ra_s.at[2, pl.ds(0, hr)], ra_s.at[2, pl.ds(hr, hr)], rb_s.at[0], rb_s.at[1], rb_s.at[2], rb_s.at[3])[i]
        return remote(src, dst, rs_send.at[i], rs_recv.at[i], peer(hops[i]))

    def cz_at(k, off, n):
        return cz_s.at[pl.ds(pl.multiple_of(chip(k) * chunk + off, 8), n)]

    def aa_copy(i):
        src = (lambda: cz_at(3, 0, chunk), lambda: cz_at(-3, 0, chunk), lambda: cz_at(4, 0, part), lambda: cz_at(4, ml_at, part),
               lambda: tw_s.at[0], lambda: tw_s.at[1], lambda: cz_at(1, 0, chunk), lambda: cz_at(-1, 0, chunk))[i]()
        dst = (ta_s.at[0], ta_s.at[1], ta_s.at[2, pl.ds(0, part)], ta_s.at[3, pl.ds(0, part)], tb_s.at[0], tb_s.at[1], tb_s.at[2], tb_s.at[3])[i]
        return remote(src, dst, aa_send.at[i], aa_recv.at[i], peer(hops[i]))

    g_hop = (2, -2, 1, -1, 1, -1, 2, -2)
    g_src = (0, 0, 0, 0, -2, 2, -2, 2)

    def gather_copy(buf, send, recv, i):
        ref = buf.at[c * chips + chip(g_src[i])]
        if i >= 6:
            ref = ref.at[pl.ds((i - 6) * hr, hr)]
        return remote(ref, ref, send.at[i], recv.at[i], peer(g_hop[i]))

    def gather_recv(buf, send, recv, i):
        ref = buf.at[c * chips + chip(g_src[i] - g_hop[i])]
        if i >= 6:
            ref = ref.at[pl.ds((i - 6) * hr, hr)]
        return remote(ref, ref, send.at[i], recv.at[i], peer(g_hop[i]))

    def ma_copy(i):
        return gather_copy(ma_s, ma_send, ma_recv, i)

    def cg_copy(i):
        return gather_copy(g_s, cg_send, cg_recv, i)

    def ma_wait(i):
        gather_recv(ma_s, ma_send, ma_recv, i).wait_recv()

    def cg_wait(i):
        gather_recv(g_s, cg_send, cg_recv, i).wait_recv()

    def ma_fwd(owner, k):
        ref = ma_s.at[owner * chips + chip(k)]
        return remote(ref, ref, mf_send.at[k % chips], mf_recv.at[k % chips], partner)

    def cg_fwd(owner, k):
        ref = g_s.at[owner * chips + chip(k)]
        return remote(ref, ref, cf_send.at[k % chips], cf_recv.at[k % chips], partner)

    ph = Phases()
    ph('entry')
    for i in range(4):
        in_copy(i).start()
    for i in range(2):
        up_copy(i).start()
    bar = pltpu.get_barrier_semaphore()
    pl.semaphore_signal(bar, inc=1, device_id=partner, device_id_type=MESH)
    for k in (1, -1, 2, -2):
        pl.semaphore_signal(bar, inc=1, device_id=peer(k), device_id_type=MESH)

    ph('in_wait')
    for i in range(4):
        in_copy(i).wait()
    for i in range(2, n_up):
        up_copy(i).start()
    for half in range(2):
        for i in range(chips):
            dn_copy(half, i).start()
    ph('layer_norm')

    @pl.loop(0, rows // 16)
    def _(i):
        sl = pl.ds(pl.multiple_of(i * 16, 16), 16)
        xf = x_s[sl, :].astype(F32)
        mean = jnp.mean(xf, axis=-1, keepdims=True)
        cen = xf - mean
        var = jnp.mean(cen * cen, axis=-1, keepdims=True)
        h_s[sl, :] = (cen * lax.rsqrt(var + LN_EPS) * gb_s[0:1, :] + gb_s[8:9, :]).astype(BF16)

    ph('rope')
    for b in range(rows):
        lp_s[b:b + 1, :] = jnp.full((1, HALF), pos_s[b], jnp.int32).astype(F32)
    ang = lp_s[...] * inv_ref[...]
    cs_s[...] = jnp.cos(ang)
    sn_s[...] = jnp.sin(ang)
    lp_s[...] = lp_s[...] - (s * seq).astype(F32)

    def chunk_dots(a_ref, bases, depth):
        accs = [None] * len(bases)
        for kk in range(depth // BLK):
            a = a_ref[:, kk * BLK:(kk + 1) * BLK]
            for j, row in enumerate(bases):
                w = w_s[pl.ds(pl.multiple_of(row + kk * BLK, BLK), BLK), :]
                p = jnp.dot(a, w, preferred_element_type=F32)
                accs[j] = p if accs[j] is None else accs[j] + p
        return accs

    ph('mlp_up')

    for i in range(0, n_up, 2):
        up_copy(i).wait()
        up_copy(i + 1).wait()
        us = chunk_dots(h_s, [(i + j) * up_rows for j in range(2)], up_rows)
        for j, u in enumerate(us):
            g = 0.5 * u * (1.0 + lax.erf(u * (0.5 ** 0.5)))
            act_s[:, (i + j) * BLK:(i + j + 1) * BLK] = g.astype(BF16)
        if i == 0:
            for n in range(3):
                qkv_copy(n).start()

    ph('barrier')
    pl.semaphore_wait(bar, 5)
    ph('down_partner')
    qkv_copy(3).start()
    for i in range(0, chips, 4):
        for j in range(4):
            dn_copy(0, i + j).wait()
        for j, p in enumerate(chunk_dots(act_s, [dn_base + (i + j) * dn_rows for j in range(4)], dn_rows)):
            ps_s[i + j] = p
            pd_copy(i + j).start()

    ph('down_own')
    for i in range(4, 6):
        qkv_copy(i).start()
    for i in range(0, chips, 4):
        for j in range(4):
            dn_copy(1, i + j).wait()
        for j, p in enumerate(chunk_dots(act_s, [dn_base + (chips + i + j) * dn_rows for j in range(4)], dn_rows)):
            n = i + j
            pd_copy(n).wait_recv()
            ss_s[n] = p + pr_s[n]
            for m in ((0,), (1,), (2, 3), (), (), (6,), (7,), ())[n]:
                rs_copy(m).start()

    def qkv_store(i, acc):
        a = acc.astype(BF16).astype(F32)
        a1, a2 = a[:, :HALF], a[:, HALF:]
        cs, sn = cs_s[...], sn_s[...]
        r1 = (a1 * cs - a2 * sn).astype(BF16).astype(F32)
        r2 = (a2 * cs + a1 * sn).astype(BF16).astype(F32)
        slot = c * slots + i
        is_v = slot == heads + 1
        row = pl.multiple_of(slot * 2 * rows, 8)
        qk_s[pl.ds(row, rows), :] = jnp.where(is_v, a1, r1)
        qk_s[pl.ds(row + rows, rows), :] = jnp.where(is_v, a2, r2)
        qx_copy(c, i).start()

    def qkv_pair(i):
        qkv_copy(2 * i).wait()
        qkv_copy(2 * i + 1).wait()
        for j, acc in enumerate(chunk_dots(h_s, [qkv_base + (2 * i + j) * d_model for j in range(2)], d_model)):
            qkv_store(2 * i + j, acc)

    n_pair = slots // 2
    ph('qkv')
    for i in range(6, slots):
        qkv_copy(i).start()
    pl.loop(0, n_pair - 1)(qkv_pair)

    for i in range(n_kv):
        kv_copy(0, i).start()
        kv_copy(1, i).start()

    ph('rs_add')
    for i in range(4):
        rs_copy(i).wait_recv()
    ss_s[3, 0:hr] = ss_s[3, 0:hr] + ra_s[0, 0:hr] + ra_s[2, 0:hr]
    ss_s[3, hr:] = ss_s[3, hr:] + ra_s[0, hr:]
    ss_s[4, 0:hr] = ss_s[4, 0:hr] + ra_s[1, 0:hr]
    ss_s[4, hr:] = ss_s[4, hr:] + ra_s[1, hr:] + ra_s[2, hr:]
    rs_copy(4).start()
    rs_copy(5).start()
    ph('qkv_last')
    qkv_pair(n_pair - 1)
    for i in range(2 * n_pair, slots):
        qkv_copy(i).wait()
        qkv_store(i, chunk_dots(h_s, [qkv_base + i * d_model], d_model)[0])

    for i in range(n_col):
        wo_copy(i).start()

    ph('qkv_wait')
    for i in range(slots):
        qx_copy(pc, i).wait_recv()
    lane = lax.broadcasted_iota(jnp.int32, (heads, seq), 1)
    lane_f = lane.astype(F32)
    scale = k_s.shape[2] ** -0.5
    group = rows // 4

    def attend(g, carry):
        mm, ll = carry
        base = g * group
        scores, values, here = [], [], []
        for r in range(group):
            b = base + r

            def both(at, n):
                return jnp.concatenate([qk_s[pl.ds(at + b, n, stride=2 * rows), :], qk_s[pl.ds(at + rows + b, n, stride=2 * rows), :]], axis=-1)

            def one(at):
                return jnp.concatenate([qk_s[pl.ds(at + b, 1), :], qk_s[pl.ds(at + rows + b, 1), :]], axis=-1)

            q = both(0, heads)
            kn = one(2 * heads * rows)
            lp = lp_s[pl.ds(b, 1), :]
            here.append(lane_f == lp)
            sc = lax.dot_general(q.astype(BF16), k_s[b], (((1,), (1,)), ((), ())), preferred_element_type=F32)
            sc = jnp.where(here[r], jnp.sum(q * kn, axis=-1, keepdims=True), sc) * scale
            scores.append(jnp.where(lane_f <= lp, sc, NEG_FILL))
            values.append(one((2 * heads + 2) * rows))
        es, news = [], []
        for r in range(group):
            m = jnp.max(scores[r], axis=-1, keepdims=True)
            e = jnp.where(lane_f <= lp_s[pl.ds(base + r, 1), :], jnp.exp(scores[r] - m), 0.0)
            col = lane == base + r
            mm = jnp.where(col, m, mm)
            ll = jnp.where(col, jnp.sum(e, axis=-1, keepdims=True), ll)
            eb = e.astype(BF16).astype(F32)
            news.append(jnp.sum(jnp.where(here[r], eb, 0.0), axis=-1, keepdims=True))
            es.append(jnp.where(here[r], 0.0, eb).astype(BF16))
        for r in range(group):
            b = base + r
            o = jnp.dot(es[r], v_s[b], preferred_element_type=F32) + news[r] * values[r]
            at = pl.ds(pl.multiple_of(b * half_heads, 8), half_heads)
            ost_s[0, at, :] = o[:half_heads]
            ost_s[1, at, :] = o[half_heads:]
        return mm, ll

    ph('kv_wait')
    for i in range(n_kv):
        kv_copy(0, i).wait()
        kv_copy(1, i).wait()
    ph('attention')
    zero = jnp.zeros((heads, seq), F32)
    mm, ll = lax.fori_loop(0, 3, attend, (zero, zero))

    ph('rs_sum')
    for i in range(4, 8):
        rs_copy(i).wait_recv()
    ma_s[c * chips + z] = ss_s[7] + rb_s[0] + rb_s[1] + rb_s[2] + rb_s[3]
    for i in range(4):
        ma_copy(i).start()
    ma_fwd(c, 0).start()

    ph('attention_last')
    mm, ll = lax.fori_loop(3, 4, attend, (mm, ll))
    ml = jnp.concatenate([mm, ll], axis=-1)
    ost_s[0, rows * half_heads:, :] = ml[:half_heads]
    ost_s[1, rows * half_heads:, :] = ml[half_heads:]
    st_copy().start()

    ph('stat_wait')
    st_copy().wait_recv()
    ph('merge')
    base = rows * half_heads
    m_s, l_s = ost_s[c, base:, :HALF], ost_s[c, base:, HALF:]
    m_p, l_p = orx_s[base:, :HALF], orx_s[base:, HALF:]
    m_c = jnp.maximum(m_s, m_p)
    w_own, w_par = jnp.exp(m_s - m_c), jnp.exp(m_p - m_c)

    def put(at, val):
        cz_s[pl.ds(at, half_heads, stride=chunk), :] = val

    for b in range(rows):
        sl = slice(b * half_heads, (b + 1) * half_heads)
        mix = ost_s[c, sl, :] * w_own[:, b:b + 1] + orx_s[sl, :] * w_par[:, b:b + 1]
        at = b if b < hr else hi_at + b - hr
        put(at, mix[:, :HALF])
        put(at + hr, mix[:, HALF:])
    put(ml_at, m_c)
    put(ml_at + 1, l_s * w_own + l_p * w_par)
    nil = jnp.zeros((half_heads, HALF), F32)
    for i in range(2, 8):
        put(ml_at + i, nil)
    for i in (2, 3, 0, 1):
        aa_copy(i).start()

    row_lane = lax.broadcasted_iota(jnp.int32, (1, HALF), 1)
    is_lo = row_lane < hr

    def blend(parts, out):
        ms, ls = [], []
        for ref, at, lo, hi in parts:
            m, l = ref[at:at + 1, :], ref[at + 1:at + 2, :]
            if lo is None:
                m, l = jnp.where(is_lo, NEG_FILL, m), jnp.where(is_lo, 0.0, l)
            if hi is None:
                m, l = jnp.where(is_lo, m, NEG_FILL), jnp.where(is_lo, l, 0.0)
            ms.append(m)
            ls.append(l)
        top = functools.reduce(jnp.maximum, ms)
        ws = [jnp.exp(m - top) for m in ms]
        l_sum = functools.reduce(lambda a, b: a + b, [l * w for l, w in zip(ls, ws)])
        pad = [jnp.zeros_like(top)] * (8 - len(parts) - 1)
        cols = jnp.transpose(jnp.concatenate(ws + [l_sum] + pad, axis=0))
        for half in range(2):
            for t in range(2):
                acc = None
                for j, (ref, at, lo, hi) in enumerate(parts):
                    off = (lo, hi)[half]
                    if off is None:
                        continue
                    term = ref[off + t * hr:off + (t + 1) * hr, :] * cols[half * hr:(half + 1) * hr, j:j + 1]
                    acc = term if acc is None else acc + term
                out(half, t, acc, cols[half * hr:(half + 1) * hr, len(parts):len(parts) + 1])
        return top, l_sum

    slot_f = lax.broadcasted_iota(jnp.int32, (seq, HALF), 0).astype(F32)

    def insert(ref, head):
        @pl.loop(0, rows)
        def _(b):
            hit = slot_f == lp_s[pl.ds(b, 1), :]
            for t in range(2):
                new = qk_s[pl.ds((2 * head + t) * rows + b, 1), :]
                sl = slice(t * HALF, (t + 1) * HALF)
                ref[b, :, sl] = jnp.where(hit, new, ref[b, :, sl].astype(F32)).astype(BF16)

    ph('insert_k')
    insert(k_s, heads)
    ph('ma_on')
    ma_wait(0)
    ma_wait(1)
    for i in range(4, 8):
        ma_copy(i).start()
    ma_wait(2)
    ma_wait(3)
    for k in (2, -2, 1, -1):
        ma_fwd(c, k).start()

    for i in (6, 7):
        aa_copy(i).start()
    ph('aa_wait')
    for i in range(4):
        aa_copy(i).wait_recv()
    ph('aa_add')
    for side, k in ((0, 2), (1, -2)):
        half_part = (ta_s.at[2], ml_at, 0, None) if side == 0 else (ta_s.at[3], 0, None, 8)

        def keep(half, t, acc, _, side=side):
            off = (0, hi_at)[half] + t * hr
            tw_s[side, off:off + hr, :] = acc

        top, l_sum = blend([(cz_at(k, 0, chunk), ml_at, 0, hi_at), (ta_s.at[side], ml_at, 0, hi_at), half_part], keep)
        tw_s[side, ml_at:ml_at + 8, :] = jnp.concatenate([top, l_sum, jnp.zeros((6, HALF), F32)], axis=0)
        aa_copy(4 + side).start()

    ph('insert_v')
    insert(v_s, heads + 1)
    ph('aa_wait2')
    for i in range(4, 8):
        aa_copy(i).wait_recv()
    ph('context')

    def finish(half, t, acc, l_col):
        g_s[c * chips + z, half * hr:(half + 1) * hr, t * HALF:(t + 1) * HALF] = (acc / l_col).astype(BF16).astype(F32)

    blend([(cz_at(0, 0, chunk), ml_at, 0, hi_at)] + [(tb_s.at[j], ml_at, 0, hi_at) for j in range(4)], finish)
    for i in range(4):
        cg_copy(i).start()
    cg_fwd(c, 0).start()

    ph('wo_wait')
    for i in range(n_col):
        wo_copy(i).wait()

    def out_dots(todo, first=False):
        lhs = [g_s[slot].astype(BF16) for slot in todo]
        for n in range(n_col):
            acc = None
            for slot, a in zip(todo, lhs):
                w = w_s[pl.ds(pl.multiple_of(n * d_model + slot * BLK, BLK), BLK), :]
                p = jnp.dot(a, w, preferred_element_type=F32)
                acc = p if acc is None else acc + p
            sl = slice(n * BLK, (n + 1) * BLK)
            acc_s[:, sl] = acc if first else acc_s[:, sl] + acc

    def mine(k):
        return c * chips + chip(k)

    def theirs(k):
        return pc * chips + chip(k)

    ph('out_0')
    out_dots([mine(0)], True)
    ph('cg_wait0')
    cg_fwd(pc, 0).wait_recv()
    ph('out_0b')
    out_dots([theirs(0)])
    ph('cg_wait1')
    cg_wait(0)
    cg_copy(6).start()
    cg_copy(4).start()
    cg_wait(1)
    cg_copy(7).start()
    cg_copy(5).start()
    cg_fwd(c, -2).start()
    cg_fwd(c, 2).start()
    cg_wait(2)
    cg_fwd(c, -1).start()
    cg_wait(3)
    cg_fwd(c, 1).start()
    ph('out_1')
    out_dots([mine(-2), mine(2), mine(-1), mine(1)])
    ph('ma_tail')
    for i in range(4, 8):
        ma_wait(i)
    for k in (3, -3, 4):
        ma_fwd(c, k).start()
    ph('cg_wait2')
    for k in (-2, 2, -1, 1):
        cg_fwd(pc, k).wait_recv()
    ph('out_2')
    out_dots([theirs(-2), theirs(2), theirs(-1), theirs(1)])
    ph('cg_wait3')
    cg_wait(4)
    cg_fwd(c, -3).start()
    cg_wait(5)
    cg_fwd(c, 3).start()
    ph('out_3')
    out_dots([mine(-3), mine(3)])
    ph('cg_wait4')
    cg_wait(6)
    cg_wait(7)
    cg_fwd(c, 4).start()
    cg_fwd(pc, -3).wait_recv()
    cg_fwd(pc, 3).wait_recv()
    ph('out_4')
    out_dots([mine(4), theirs(-3), theirs(3)])
    ph('cg_wait5')
    cg_fwd(pc, 4).wait_recv()
    ph('out_5')
    out_dots([theirs(4)])
    ph('final')
    for k in range(chips):
        ma_fwd(pc, k).wait_recv()
    for n in range(n_col):
        sl = slice(n * BLK, (n + 1) * BLK)
        out_ref[:, sl] = (x_s[:, sl].astype(F32) + acc_s[:, sl] + ma_s[n]).astype(BF16)

    ph('drain')
    for i in range(chips):
        pd_copy(i).wait_send()
        ma_fwd(c, i).wait_send()
        cg_fwd(c, i).wait_send()
    for i in range(8):
        rs_copy(i).wait_send()
        aa_copy(i).wait_send()
        ma_copy(i).wait_send()
        cg_copy(i).wait_send()
    for i in range(slots):
        qx_copy(c, i).wait_send()
    st_copy().wait_send()
    ph(None)


def store_kernel(*refs):
    srcs, dsts, sem = refs[:3], refs[3:6], refs[6]
    copies = []
    for n, (src, dst) in enumerate(zip(srcs, dsts)):
        parts = 1 if n == 0 else 4
        step = src.shape[0] // parts
        for i in range(parts):
            sl = pl.ds(i * step, step)
            copies.append(pltpu.make_async_copy(src.at[sl], dst.at[sl], sem.at[n, i]))
    for copy in copies:
        copy.start()
    for copy in copies:
        copy.wait()


def device_step(n_sp, hidden, ln_gamma, ln_beta, w_qkv, w_out, w_up, w_down, k_cache, v_cache, positions):
    rows, d_model = hidden.shape
    seq, head_dim = k_cache.shape[1], k_cache.shape[2]
    heads = w_out.shape[0] // head_dim
    ff = w_up.shape[1]
    chips = n_sp // 2
    slots = (heads + 2) // 2
    assert head_dim == BLK and heads == n_sp and d_model == n_sp * BLK and chips == 8
    inv_freq = 1.0 / (ROPE_BASE ** (jnp.arange(0, head_dim, 2, dtype=F32) / head_dim))
    n_up, n_col = ff // BLK, d_model // BLK
    w_rows = n_up * d_model + n_col * ff + slots * d_model
    n_kv = 3
    half = heads // 2
    any_spec = pl.BlockSpec(memory_space=pltpu.HBM)
    vmem_spec = pl.BlockSpec(memory_space=pltpu.VMEM)
    dma = pltpu.SemaphoreType.DMA
    hr = rows // 2
    chunk, part = 4 * hr + 8, 2 * hr + 8
    scratch = [
        pltpu.VMEM((rows, d_model), BF16),
        pltpu.VMEM((16, d_model), F32),
        pltpu.VMEM((rows, d_model), BF16),
        pltpu.VMEM((rows, ff), BF16),
        pltpu.VMEM((w_rows, BLK), BF16),
        pltpu.SMEM((rows,), jnp.int32),
        pltpu.VMEM((rows, HALF), F32),
        pltpu.VMEM((rows, HALF), F32),
        pltpu.VMEM((rows, HALF), F32),
        pltpu.VMEM(((heads + 2) * 2 * rows, HALF), F32),
        pltpu.VMEM((chips, rows, BLK), F32),
        pltpu.VMEM((chips, rows, BLK), F32),
        pltpu.VMEM((chips, rows, BLK), F32),
        pltpu.VMEM((3, rows, BLK), F32),
        pltpu.VMEM((4, rows, BLK), F32),
        pltpu.VMEM((n_sp, rows, BLK), F32),
        pltpu.VMEM((2, (rows + 1) * half, BLK), F32),
        pltpu.VMEM(((rows + 1) * half, BLK), F32),
        pltpu.VMEM((chips * chunk, HALF), F32),
        pltpu.VMEM((4, chunk, HALF), F32),
        pltpu.VMEM((4, chunk, HALF), F32),
        pltpu.VMEM((2, chunk, HALF), F32),
        pltpu.VMEM((n_sp, rows, BLK), F32),
        pltpu.VMEM((rows, d_model), F32),
        dma((4,)), dma((n_up,)), dma((n_col,)), dma((slots,)), dma((2, n_kv)), dma((n_col,)),
        dma((chips,)), dma((chips,)), dma((slots,)), dma((slots,)), dma((1,)), dma((1,)),
    ] + [dma((8,))] * 12
    in_hbm = [pltpu.with_memory_space_constraint(a, pltpu.HBM) for a in (hidden, ln_gamma.reshape(1, -1), ln_beta.reshape(1, -1))]
    results = pl.pallas_call(
        functools.partial(layer_kernel, chips, heads),
        out_shape=(pltpu.VMEM(hidden.shape, BF16), pltpu.VMEM(k_cache.shape, BF16), pltpu.VMEM(v_cache.shape, BF16)),
        in_specs=[any_spec] * 10 + [vmem_spec],
        out_specs=(vmem_spec, vmem_spec, vmem_spec),
        scratch_shapes=scratch,
        compiler_params=pltpu.CompilerParams(collective_id=0, has_side_effects=True, vmem_limit_bytes=46 * 1024 * 1024),
        name='decode_layer',
    )(*in_hbm, w_qkv, w_out, w_up, w_down, k_cache, v_cache, pltpu.with_memory_space_constraint(positions, pltpu.HBM), inv_freq.reshape(1, -1))
    return pl.pallas_call(
        store_kernel,
        out_shape=[jax.ShapeDtypeStruct(r.shape, r.dtype) for r in results],
        in_specs=[vmem_spec] * 3,
        out_specs=[pl.BlockSpec(memory_space=pltpu.HBM)] * 3,
        scratch_shapes=[dma((3, 4))],
        compiler_params=pltpu.CompilerParams(vmem_limit_bytes=1024 * 1024),
        name='store_results',
    )(*results)


def solution(mesh):
    cache_spec = P('dp', 'sp', None)
    in_specs = (P('dp', None), P(None), P(None), P(None, None), P(None, None), P(None, 'sp'), P('sp', None), cache_spec, cache_spec, P('dp'))
    out_specs = (P('dp', None), cache_spec, cache_spec)
    return jax.shard_map(functools.partial(device_step, mesh.shape['sp']), mesh=mesh, in_specs=in_specs, out_specs=out_specs, check_vma=False)
```

```python
import functools

import jax
import jax.numpy as jnp
from jax import lax
from jax.experimental import pallas as pl
from jax.experimental.pallas import tpu as pltpu
from jax.sharding import PartitionSpec as P

LN_EPS = 1e-5
ROPE_BASE = 10000.0
NEG_FILL = -1e30
MESH = pl.DeviceIdType.MESH
BLK = 256
HALF = 128
F32 = jnp.float32
BF16 = jnp.bfloat16


ORDER = (3, -3, 4, 2, -2, 1, -1, 0)


class Phases:
    def __init__(self):
        self.scope = None

    def __call__(self, name):
        if self.scope is not None:
            self.scope.__exit__(None, None, None)
        self.scope = jax.named_scope(name) if name else None
        if self.scope is not None:
            self.scope.__enter__()


def layer_kernel(chips, heads, x_hbm, gamma_hbm, beta_hbm, wqkv_hbm, wout_hbm, wup_hbm, wdown_hbm, k_hbm, v_hbm, pos_hbm,
                 inv_ref, out_ref, k_s, v_s,
                 x_s, gb_s, h_s, act_s, w_s, pos_s, lp_s, cs_s, sn_s, qk_s,
                 ps_s, pr_s, ss_s, ra_s, rb_s, ma_s, ost_s, orx_s, cz_s, ta_s, tb_s, tw_s, g_s, acc_s,
                 in_sem, up_sem, dn_sem, qkv_sem, kv_sem, wo_sem,
                 pd_send, pd_recv, qx_send, qx_recv, st_send, st_recv,
                 rs_send, rs_recv, aa_send, aa_recv, ma_send, ma_recv, mf_send, mf_recv, cg_send, cg_recv, cf_send, cf_recv):
    rows, d_model = x_hbm.shape
    ff = wup_hbm.shape[1]
    seq = k_hbm.shape[1]
    n_up = ff // BLK
    n_col = d_model // BLK
    half_heads = heads // 2
    slots = (heads + 2) // 2
    hr = rows // 2
    ml_at = 2 * hr
    chunk = 2 * hr + 8
    top_rows = hr * half_heads
    up_rows, dn_rows = d_model, ff
    dn_base = n_up * up_rows
    qkv_base = dn_base + n_col * dn_rows
    n_kv = kv_sem.shape[1]
    kv_rows = rows // n_kv

    s = lax.axis_index('sp')
    z = lax.div(s, 2)
    c = lax.rem(s, 2)
    pc = 1 - c
    partner = {'sp': 2 * z + pc}

    def chip(k):
        return lax.rem(z + (k % chips), chips)

    def peer(k):
        return {'sp': 2 * chip(k) + c}

    def in_copy(i):
        src, dst = ((x_hbm, x_s), (gamma_hbm, gb_s.at[pl.ds(0, 1)]), (beta_hbm, gb_s.at[pl.ds(8, 1)]), (pos_hbm, pos_s))[i]
        return pltpu.make_async_copy(src, dst, in_sem.at[i])

    def up_copy(i):
        col = pl.multiple_of(i * BLK, BLK)
        row = pl.multiple_of(i * up_rows, BLK)
        return pltpu.make_async_copy(wup_hbm.at[:, pl.ds(col, BLK)], w_s.at[pl.ds(row, up_rows)], up_sem.at[i])

    def dn_copy(half, i):
        owner = pc if half == 0 else c
        col = pl.multiple_of((owner * chips + chip(ORDER[i])) * BLK, BLK)
        slot = half * chips + i
        row = pl.multiple_of(dn_base + slot * dn_rows, BLK)
        return pltpu.make_async_copy(wdown_hbm.at[:, pl.ds(col, BLK)], w_s.at[pl.ds(row, dn_rows)], dn_sem.at[slot])

    def qkv_copy(i):
        col = pl.multiple_of((c * slots + i) * BLK, BLK)
        row = pl.multiple_of(qkv_base + i * d_model, BLK)
        return pltpu.make_async_copy(wqkv_hbm.at[:, pl.ds(col, BLK)], w_s.at[pl.ds(row, d_model)], qkv_sem.at[i])

    def kv_copy(t, i):
        src, dst = ((k_hbm, k_s), (v_hbm, v_s))[t]
        sl = pl.ds(i * kv_rows, kv_rows)
        return pltpu.make_async_copy(src.at[sl], dst.at[sl], kv_sem.at[t, i])

    def wo_copy(i):
        col = pl.multiple_of(i * BLK, BLK)
        row = pl.multiple_of(i * d_model, BLK)
        return pltpu.make_async_copy(wout_hbm.at[:, pl.ds(col, BLK)], w_s.at[pl.ds(row, d_model)], wo_sem.at[i])

    def remote(src, dst, send, recv, to):
        return pltpu.make_async_remote_copy(src, dst, send, recv, device_id=to, device_id_type=MESH)

    def pd_copy(i):
        return remote(ps_s.at[i], pr_s.at[i], pd_send.at[i], pd_recv.at[i], partner)

    def qx_copy(owner, i):
        row = pl.multiple_of((owner * slots + i) * 2 * rows, 8)
        ref = qk_s.at[pl.ds(row, 2 * rows)]
        return remote(ref, ref, qx_send.at[i], qx_recv.at[i], partner)

    def st_copy(h):
        return remote(ost_s.at[pc, h], orx_s.at[h], st_send.at[h], st_recv.at[h], partner)

    hops = (1, -1, 2, -2, 2, -2, 1, -1)

    def rs_copy(i):
        src = (ss_s.at[0], ss_s.at[1], ss_s.at[2, pl.ds(0, hr)], ss_s.at[2, pl.ds(hr, hr)], ss_s.at[3], ss_s.at[4], ss_s.at[5], ss_s.at[6])[i]
        dst = (ra_s.at[0], ra_s.at[1], ra_s.at[2, pl.ds(0, hr)], ra_s.at[2, pl.ds(hr, hr)], rb_s.at[0], rb_s.at[1], rb_s.at[2], rb_s.at[3])[i]
        return remote(src, dst, rs_send.at[i], rs_recv.at[i], peer(hops[i]))

    def cz_at(h, k):
        return cz_s.at[pl.ds(pl.multiple_of((h * chips + chip(k)) * chunk, 8), chunk)]

    def aa_copy(h, i):
        src = (lambda: cz_at(h, 3), lambda: cz_at(h, -3), lambda: cz_at(h, 4), lambda: tw_s.at[h, 0], lambda: tw_s.at[h, 1],
               lambda: cz_at(h, 1), lambda: cz_at(h, -1))[i]()
        dst = ta_s.at[h, i] if i < 3 else tb_s.at[h, i - 3]
        hop = (1, -1, (2, -2)[h], 2, -2, 1, -1)[i]
        return remote(src, dst, aa_send.at[7 * h + i], aa_recv.at[7 * h + i], peer(hop))

    g_hop = (2, -2, 1, -1, 1, -1, 2, -2)
    g_src = (0, 0, 0, 0, -2, 2, -2, 2)

    def gather_copy(buf, send, recv, i):
        ref = buf.at[c * chips + chip(g_src[i])]
        if i >= 6:
            ref = ref.at[pl.ds((i - 6) * hr, hr)]
        return remote(ref, ref, send.at[i], recv.at[i], peer(g_hop[i]))

    def gather_recv(buf, send, recv, i):
        ref = buf.at[c * chips + chip(g_src[i] - g_hop[i])]
        if i >= 6:
            ref = ref.at[pl.ds((i - 6) * hr, hr)]
        return remote(ref, ref, send.at[i], recv.at[i], peer(g_hop[i]))

    def ma_copy(i):
        return gather_copy(ma_s, ma_send, ma_recv, i)

    def cg_route(h, i):
        return ((0, 2), (0, -2), (0, 1), (0, -1), (-2, 1), (2, -1), ((-2, 2), (2, -2))[h])[i]

    def cg_part(h, i, k, hop):
        ref = g_s.at[c * chips + chip(k), pl.ds(h * hr, hr)]
        return remote(ref, ref, cg_send.at[7 * h + i], cg_recv.at[7 * h + i], peer(hop))

    def cg_copy(h, i):
        src, hop = cg_route(h, i)
        return cg_part(h, i, src, hop)

    def ma_wait(i):
        gather_recv(ma_s, ma_send, ma_recv, i).wait_recv()

    def cg_wait(h, i):
        src, hop = cg_route(h, i)
        cg_part(h, i, src - hop, hop).wait_recv()

    def ma_fwd(owner, k):
        ref = ma_s.at[owner * chips + chip(k)]
        return remote(ref, ref, mf_send.at[k % chips], mf_recv.at[k % chips], partner)

    def cg_fwd(owner, k):
        ref = g_s.at[owner * chips + chip(k)]
        return remote(ref, ref, cf_send.at[k % chips], cf_recv.at[k % chips], partner)

    ph = Phases()
    ph('entry')
    for i in range(4):
        in_copy(i).start()
    for i in range(2):
        qkv_copy(i).start()
    bar = pltpu.get_barrier_semaphore()
    pl.semaphore_signal(bar, inc=1, device_id=partner, device_id_type=MESH)
    for k in (1, -1, 2, -2):
        pl.semaphore_signal(bar, inc=1, device_id=peer(k), device_id_type=MESH)

    ph('in_wait')
    for i in range(4):
        in_copy(i).wait()
    for i in range(2, slots):
        qkv_copy(i).start()
    ph('layer_norm')

    @pl.loop(0, rows // 16)
    def _(i):
        sl = pl.ds(pl.multiple_of(i * 16, 16), 16)
        xf = x_s[sl, :].astype(F32)
        mean = jnp.mean(xf, axis=-1, keepdims=True)
        cen = xf - mean
        var = jnp.mean(cen * cen, axis=-1, keepdims=True)
        h_s[sl, :] = (cen * lax.rsqrt(var + LN_EPS) * gb_s[0:1, :] + gb_s[8:9, :]).astype(BF16)

    nil = jnp.zeros((half_heads, HALF), F32)
    for h in range(2):
        for i in range(ml_at + 2, chunk):
            cz_s[pl.ds(h * chips * chunk + i, half_heads, stride=chunk), :] = nil
    ph('rope')
    for b in range(rows):
        lp_s[b:b + 1, :] = jnp.full((1, HALF), pos_s[b], jnp.int32).astype(F32)
    ang = lp_s[...] * inv_ref[...]
    cs_s[...] = jnp.cos(ang)
    sn_s[...] = jnp.sin(ang)
    lp_s[...] = lp_s[...] - (s * seq).astype(F32)

    def chunk_dots(a_ref, bases, depth):
        accs = [None] * len(bases)
        for kk in range(depth // BLK):
            a = a_ref[:, kk * BLK:(kk + 1) * BLK]
            for j, row in enumerate(bases):
                w = w_s[pl.ds(pl.multiple_of(row + kk * BLK, BLK), BLK), :]
                p = jnp.dot(a, w, preferred_element_type=F32)
                accs[j] = p if accs[j] is None else accs[j] + p
        return accs

    def qkv_store(i, acc, send=True):
        a = acc.astype(BF16).astype(F32)
        a1, a2 = a[:, :HALF], a[:, HALF:]
        cs, sn = cs_s[...], sn_s[...]
        r1 = (a1 * cs - a2 * sn).astype(BF16).astype(F32)
        r2 = (a2 * cs + a1 * sn).astype(BF16).astype(F32)
        slot = c * slots + i
        is_v = slot == heads + 1
        row = pl.multiple_of(slot * 2 * rows, 8)
        qk_s[pl.ds(row, rows), :] = jnp.where(is_v, a1, r1)
        qk_s[pl.ds(row + rows, rows), :] = jnp.where(is_v, a2, r2)
        if send:
            qx_copy(c, i).start()

    def qkv_pair(i, send=True):
        qkv_copy(2 * i).wait()
        qkv_copy(2 * i + 1).wait()
        for j, acc in enumerate(chunk_dots(h_s, [qkv_base + (2 * i + j) * d_model for j in range(2)], d_model)):
            qkv_store(2 * i + j, acc, send)

    n_pair = slots // 2
    ph('qkv')
    qkv_pair(0, False)
    ph('barrier')
    pl.semaphore_wait(bar, 5)
    ph('qkv2')
    for i in range(2):
        qx_copy(c, i).start()
    pl.loop(1, n_pair - 1)(qkv_pair)
    for i in range(n_kv):
        kv_copy(0, i).start()
        kv_copy(1, i).start()

    ph('qkv_last')
    qkv_pair(n_pair - 1)
    for i in range(2 * n_pair, slots):
        qkv_copy(i).wait()
        qkv_store(i, chunk_dots(h_s, [qkv_base + i * d_model], d_model)[0])

    ph('qkv_wait')
    for i in range(slots):
        qx_copy(pc, i).wait_recv()
    lane = lax.broadcasted_iota(jnp.int32, (heads, seq), 1)
    lane_f = lane.astype(F32)
    scale = k_s.shape[2] ** -0.5
    group = rows // 4

    def attend(h, g, carry):
        mm, ll = carry
        base = g * group
        kv_copy(0, g).wait()
        kv_copy(1, g).wait()
        scores, values, here = [], [], []
        for r in range(group):
            b = base + r

            def both(at, n):
                return jnp.concatenate([qk_s[pl.ds(at + b, n, stride=2 * rows), :], qk_s[pl.ds(at + rows + b, n, stride=2 * rows), :]], axis=-1)

            def one(at):
                return jnp.concatenate([qk_s[pl.ds(at + b, 1), :], qk_s[pl.ds(at + rows + b, 1), :]], axis=-1)

            q = both(0, heads)
            kn = one(2 * heads * rows)
            lp = lp_s[pl.ds(b, 1), :]
            here.append(lane_f == lp)
            sc = lax.dot_general(q.astype(BF16), k_s[b], (((1,), (1,)), ((), ())), preferred_element_type=F32)
            sc = jnp.where(here[r], jnp.sum(q * kn, axis=-1, keepdims=True), sc) * scale
            scores.append(jnp.where(lane_f <= lp, sc, NEG_FILL))
            values.append(one((2 * heads + 2) * rows))
        es, news = [], []
        for r in range(group):
            m = jnp.max(scores[r], axis=-1, keepdims=True)
            e = jnp.where(lane_f <= lp_s[pl.ds(base + r, 1), :], jnp.exp(scores[r] - m), 0.0)
            col = lane == base + r - h * hr
            mm = jnp.where(col, m, mm)
            ll = jnp.where(col, jnp.sum(e, axis=-1, keepdims=True), ll)
            eb = e.astype(BF16).astype(F32)
            news.append(jnp.sum(jnp.where(here[r], eb, 0.0), axis=-1, keepdims=True))
            es.append(jnp.where(here[r], 0.0, eb).astype(BF16))
        for r in range(group):
            b = base + r
            o = jnp.dot(es[r], v_s[b], preferred_element_type=F32) + news[r] * values[r]
            at = pl.ds(pl.multiple_of((b - h * hr) * half_heads, 8), half_heads)
            ost_s[0, h, at, :] = o[:half_heads]
            ost_s[1, h, at, :] = o[half_heads:]
        return mm, ll

    def attend_half(h):
        zero = jnp.zeros((heads, seq), F32)
        mm, ll = lax.fori_loop(2 * h, 2 * h + 2, functools.partial(attend, h), (zero, zero))
        ml = jnp.concatenate([mm, ll], axis=-1)
        ost_s[0, h, top_rows:, :] = ml[:half_heads]
        ost_s[1, h, top_rows:, :] = ml[half_heads:]
        st_copy(h).start()

    ph('attention')
    for i in range(n_up):
        up_copy(i).start()
    attend_half(0)

    ph('attention_last')
    attend_half(1)
    for half in range(2):
        for i in range(chips):
            dn_copy(half, i).start()

    def merge(h):
        m_s, l_s = ost_s[c, h, top_rows:, :HALF], ost_s[c, h, top_rows:, HALF:]
        m_p, l_p = orx_s[h, top_rows:, :HALF], orx_s[h, top_rows:, HALF:]
        m_c = jnp.maximum(m_s, m_p)
        w_own, w_par = jnp.exp(m_s - m_c), jnp.exp(m_p - m_c)

        def put(at, val):
            cz_s[pl.ds(h * chips * chunk + at, half_heads, stride=chunk), :] = val

        for b in range(hr):
            sl = slice(b * half_heads, (b + 1) * half_heads)
            mix = ost_s[c, h, sl, :] * w_own[:, b:b + 1] + orx_s[h, sl, :] * w_par[:, b:b + 1]
            put(b, mix[:, :HALF])
            put(hr + b, mix[:, HALF:])
        put(ml_at, m_c)
        put(ml_at + 1, l_s * w_own + l_p * w_par)

    def mlp_up(i):
        up_copy(i).wait()
        up_copy(i + 1).wait()
        us = chunk_dots(h_s, [(i + j) * up_rows for j in range(2)], up_rows)
        for j, u in enumerate(us):
            g = 0.5 * u * (1.0 + lax.erf(u * (0.5 ** 0.5)))
            act_s[:, (i + j) * BLK:(i + j + 1) * BLK] = g.astype(BF16)

    def blend(refs, out):
        ms = [ref[ml_at:ml_at + 1, :] for ref in refs]
        ls = [ref[ml_at + 1:ml_at + 2, :] for ref in refs]
        top = functools.reduce(jnp.maximum, ms)
        ws = [jnp.exp(m - top) for m in ms]
        l_sum = functools.reduce(lambda a, b: a + b, [l * w for l, w in zip(ls, ws)])
        pad = [jnp.zeros_like(top)] * (8 - len(refs) - 1)
        cols = jnp.transpose(jnp.concatenate(ws + [l_sum] + pad, axis=0))[:hr]
        for t in range(2):
            terms = [ref[t * hr:(t + 1) * hr, :] * cols[:, j:j + 1] for j, ref in enumerate(refs)]
            out(t, functools.reduce(lambda a, b: a + b, terms), cols[:, len(refs):len(refs) + 1])
        return top, l_sum

    slot_f = lax.broadcasted_iota(jnp.int32, (seq, HALF), 0).astype(F32)

    def insert(ref, head):
        @pl.loop(0, rows)
        def _(b):
            hit = slot_f == lp_s[pl.ds(b, 1), :]
            for t in range(2):
                new = qk_s[pl.ds((2 * head + t) * rows + b, 1), :]
                sl = slice(t * HALF, (t + 1) * HALF)
                ref[b, :, sl] = jnp.where(hit, new, ref[b, :, sl].astype(F32)).astype(BF16)

    for h in range(2):
        ph(f'stat_wait{h}')
        st_copy(h).wait_recv()
        ph(f'merge{h}')
        merge(h)
        for i in (2, 0, 1):
            aa_copy(h, i).start()
        ph(f'mlp_up{h}')
        if h == 1:
            for k in range(2):
                for i in (5, 6):
                    aa_copy(k, i).start()
            for i in range(n_col // 2, n_col):
                wo_copy(i).start()
        mlp_up(h * n_up // 2)
    ph('down_partner')
    for i in range(0, chips, 4):
        for j in range(4):
            dn_copy(0, i + j).wait()
        for j, p in enumerate(chunk_dots(act_s, [dn_base + (i + j) * dn_rows for j in range(4)], dn_rows)):
            ps_s[i + j] = p
            pd_copy(i + j).start()

    ph('down_own')
    for i in range(0, chips, 4):
        for j in range(4):
            dn_copy(1, i + j).wait()
        for j, p in enumerate(chunk_dots(act_s, [dn_base + (chips + i + j) * dn_rows for j in range(4)], dn_rows)):
            n = i + j
            pd_copy(n).wait_recv()
            ss_s[n] = p + pr_s[n]
            for m in ((0,), (1,), (2, 3), (), (), (6,), (7,), ())[n]:
                rs_copy(m).start()

    for i in range(n_col // 2):
        wo_copy(i).start()
    for h in range(2):
        ph(f'aa_wait{h}')
        for i in range(3):
            aa_copy(h, i).wait_recv()
        ph(f'aa_add{h}')
        for side in range(2):
            def keep(t, acc, _):
                tw_s[h, side, t * hr:(t + 1) * hr, :] = acc

            more = [ta_s.at[h, 2]] if side == h else []
            top, l_sum = blend([cz_at(h, (2, -2)[side]), ta_s.at[h, side]] + more, keep)
            tw_s[h, side, ml_at:, :] = jnp.concatenate([top, l_sum, jnp.zeros((6, HALF), F32)], axis=0)
            aa_copy(h, 3 + side).start()
    ph('insert_k')
    insert(k_s, heads)
    ph('rs_add')
    for i in range(4):
        rs_copy(i).wait_recv()
    ss_s[3, 0:hr] = ss_s[3, 0:hr] + ra_s[0, 0:hr] + ra_s[2, 0:hr]
    ss_s[3, hr:] = ss_s[3, hr:] + ra_s[0, hr:]
    ss_s[4, 0:hr] = ss_s[4, 0:hr] + ra_s[1, 0:hr]
    ss_s[4, hr:] = ss_s[4, hr:] + ra_s[1, hr:] + ra_s[2, hr:]
    rs_copy(4).start()
    rs_copy(5).start()
    ph('insert_v')
    insert(v_s, heads + 1)
    for h in range(2):
        ph(f'aa_last{h}')
        for i in range(3, 7):
            aa_copy(h, i).wait_recv()
        ph(f'context{h}')

        def finish(t, acc, l_col):
            g_s[c * chips + z, h * hr:(h + 1) * hr, t * HALF:(t + 1) * HALF] = (acc / l_col).astype(BF16).astype(F32)

        blend([cz_at(h, 0)] + [tb_s.at[h, j] for j in range(4)], finish)
        for i in range(4):
            cg_copy(h, i).start()
    cg_fwd(c, 0).start()

    ph('rs_sum')
    for i in range(4, 8):
        rs_copy(i).wait_recv()
    ma_s[c * chips + z] = ss_s[7] + rb_s[0] + rb_s[1] + rb_s[2] + rb_s[3]
    for i in range(4):
        ma_copy(i).start()
    ma_fwd(c, 0).start()

    ph('wo_wait')
    for i in range(n_col):
        wo_copy(i).wait()

    def out_dots(todo, first=False):
        lhs = [g_s[slot].astype(BF16) for slot in todo]
        for n in range(n_col):
            acc = None
            for slot, a in zip(todo, lhs):
                w = w_s[pl.ds(pl.multiple_of(n * d_model + slot * BLK, BLK), BLK), :]
                p = jnp.dot(a, w, preferred_element_type=F32)
                acc = p if acc is None else acc + p
            sl = slice(n * BLK, (n + 1) * BLK)
            acc_s[:, sl] = acc if first else acc_s[:, sl] + acc

    def mine(k):
        return c * chips + chip(k)

    def theirs(k):
        return pc * chips + chip(k)

    ph('out_0')
    out_dots([mine(0)], True)
    ph('cg_wait0')
    cg_fwd(pc, 0).wait_recv()
    ph('out_0b')
    out_dots([theirs(0)])
    ph('cg_wait1')
    for h in range(2):
        cg_wait(h, 0)
        if h == 0:
            cg_copy(0, 6).start()
        cg_copy(h, 4).start()
        cg_wait(h, 1)
        if h == 1:
            cg_copy(1, 6).start()
        cg_copy(h, 5).start()
    cg_fwd(c, -2).start()
    cg_fwd(c, 2).start()
    cg_wait(0, 2)
    cg_wait(1, 2)
    cg_fwd(c, -1).start()
    cg_wait(0, 3)
    cg_wait(1, 3)
    cg_fwd(c, 1).start()
    ph('out_1')
    out_dots([mine(-2), mine(2), mine(-1), mine(1)])
    ph('ma_on')
    ma_wait(0)
    ma_wait(1)
    for i in range(4, 8):
        ma_copy(i).start()
    ma_wait(2)
    ma_wait(3)
    for k in (2, -2, 1, -1):
        ma_fwd(c, k).start()

    ph('cg_wait2')
    for k in (-2, 2, -1, 1):
        cg_fwd(pc, k).wait_recv()
    ph('out_2')
    out_dots([theirs(-2), theirs(2), theirs(-1), theirs(1)])
    ph('cg_wait3')
    cg_wait(0, 4)
    cg_wait(1, 4)
    cg_fwd(c, -3).start()
    cg_wait(0, 5)
    cg_wait(1, 5)
    cg_fwd(c, 3).start()
    ph('out_3')
    out_dots([mine(-3), mine(3)])
    ph('cg_wait4')
    cg_wait(0, 6)
    cg_wait(1, 6)
    cg_fwd(c, 4).start()
    cg_fwd(pc, -3).wait_recv()
    cg_fwd(pc, 3).wait_recv()
    ph('out_4')
    out_dots([mine(4), theirs(-3), theirs(3)])
    ph('ma_tail')
    for i in range(4, 8):
        ma_wait(i)
    for k in (3, -3, 4):
        ma_fwd(c, k).start()
    ph('cg_wait5')
    cg_fwd(pc, 4).wait_recv()
    ph('out_5')
    out_dots([theirs(4)])
    ph('final')
    for k in range(chips):
        ma_fwd(pc, k).wait_recv()
    for n in range(n_col):
        sl = slice(n * BLK, (n + 1) * BLK)
        out_ref[:, sl] = (x_s[:, sl].astype(F32) + acc_s[:, sl] + ma_s[n]).astype(BF16)

    ph('drain')
    for i in range(chips):
        pd_copy(i).wait_send()
        ma_fwd(c, i).wait_send()
        cg_fwd(c, i).wait_send()
    for i in range(8):
        rs_copy(i).wait_send()
        ma_copy(i).wait_send()
    for h in range(2):
        st_copy(h).wait_send()
        for i in range(7):
            aa_copy(h, i).wait_send()
            cg_copy(h, i).wait_send()
    for i in range(slots):
        qx_copy(c, i).wait_send()
    ph(None)


def store_kernel(*refs):
    srcs, dsts, sem = refs[:3], refs[3:6], refs[6]
    copies = []
    for n, (src, dst) in enumerate(zip(srcs, dsts)):
        parts = 1 if n == 0 else 4
        step = src.shape[0] // parts
        for i in range(parts):
            sl = pl.ds(i * step, step)
            copies.append(pltpu.make_async_copy(src.at[sl], dst.at[sl], sem.at[n, i]))
    for copy in copies:
        copy.start()
    for copy in copies:
        copy.wait()


def device_step(n_sp, hidden, ln_gamma, ln_beta, w_qkv, w_out, w_up, w_down, k_cache, v_cache, positions):
    rows, d_model = hidden.shape
    seq, head_dim = k_cache.shape[1], k_cache.shape[2]
    heads = w_out.shape[0] // head_dim
    ff = w_up.shape[1]
    chips = n_sp // 2
    slots = (heads + 2) // 2
    assert head_dim == BLK and heads == n_sp and d_model == n_sp * BLK and chips == 8
    inv_freq = 1.0 / (ROPE_BASE ** (jnp.arange(0, head_dim, 2, dtype=F32) / head_dim))
    n_up, n_col = ff // BLK, d_model // BLK
    w_rows = n_up * d_model + n_col * ff + slots * d_model
    n_kv = 4
    half = heads // 2
    any_spec = pl.BlockSpec(memory_space=pltpu.HBM)
    vmem_spec = pl.BlockSpec(memory_space=pltpu.VMEM)
    dma = pltpu.SemaphoreType.DMA
    hr = rows // 2
    chunk = 2 * hr + 8
    scratch = [
        pltpu.VMEM((rows, d_model), BF16),
        pltpu.VMEM((16, d_model), F32),
        pltpu.VMEM((rows, d_model), BF16),
        pltpu.VMEM((rows, ff), BF16),
        pltpu.VMEM((w_rows, BLK), BF16),
        pltpu.SMEM((rows,), jnp.int32),
        pltpu.VMEM((rows, HALF), F32),
        pltpu.VMEM((rows, HALF), F32),
        pltpu.VMEM((rows, HALF), F32),
        pltpu.VMEM(((heads + 2) * 2 * rows, HALF), F32),
        pltpu.VMEM((chips, rows, BLK), F32),
        pltpu.VMEM((chips, rows, BLK), F32),
        pltpu.VMEM((chips, rows, BLK), F32),
        pltpu.VMEM((3, rows, BLK), F32),
        pltpu.VMEM((4, rows, BLK), F32),
        pltpu.VMEM((n_sp, rows, BLK), F32),
        pltpu.VMEM((2, 2, (hr + 1) * half, BLK), F32),
        pltpu.VMEM((2, (hr + 1) * half, BLK), F32),
        pltpu.VMEM((2 * chips * chunk, HALF), F32),
        pltpu.VMEM((2, 3, chunk, HALF), F32),
        pltpu.VMEM((2, 4, chunk, HALF), F32),
        pltpu.VMEM((2, 2, chunk, HALF), F32),
        pltpu.VMEM((n_sp, rows, BLK), F32),
        pltpu.VMEM((rows, d_model), F32),
        dma((4,)), dma((n_up,)), dma((n_col,)), dma((slots,)), dma((2, n_kv)), dma((n_col,)),
        dma((chips,)), dma((chips,)), dma((slots,)), dma((slots,)), dma((2,)), dma((2,)),
    ] + [dma((n,)) for n in (8, 8, 14, 14, 8, 8, 8, 8, 14, 14, 8, 8)]
    in_hbm = [pltpu.with_memory_space_constraint(a, pltpu.HBM) for a in (hidden, ln_gamma.reshape(1, -1), ln_beta.reshape(1, -1))]
    results = pl.pallas_call(
        functools.partial(layer_kernel, chips, heads),
        out_shape=(pltpu.VMEM(hidden.shape, BF16), pltpu.VMEM(k_cache.shape, BF16), pltpu.VMEM(v_cache.shape, BF16)),
        in_specs=[any_spec] * 10 + [vmem_spec],
        out_specs=(vmem_spec, vmem_spec, vmem_spec),
        scratch_shapes=scratch,
        compiler_params=pltpu.CompilerParams(collective_id=0, has_side_effects=True, vmem_limit_bytes=46 * 1024 * 1024),
        name='decode_layer',
    )(*in_hbm, w_qkv, w_out, w_up, w_down, k_cache, v_cache, pltpu.with_memory_space_constraint(positions, pltpu.HBM), inv_freq.reshape(1, -1))
    return pl.pallas_call(
        store_kernel,
        out_shape=[jax.ShapeDtypeStruct(r.shape, r.dtype) for r in results],
        in_specs=[vmem_spec] * 3,
        out_specs=[pl.BlockSpec(memory_space=pltpu.HBM)] * 3,
        scratch_shapes=[dma((3, 4))],
        compiler_params=pltpu.CompilerParams(vmem_limit_bytes=1024 * 1024),
        name='store_results',
    )(*results)


def solution(mesh):
    cache_spec = P('dp', 'sp', None)
    in_specs = (P('dp', None), P(None), P(None), P(None, None), P(None, None), P(None, 'sp'), P('sp', None), cache_spec, cache_spec, P('dp'))
    out_specs = (P('dp', None), cache_spec, cache_spec)
    return jax.shard_map(functools.partial(device_step, mesh.shape['sp']), mesh=mesh, in_specs=in_specs, out_specs=out_specs, check_vma=False)
```

```python
import functools

import jax
import jax.numpy as jnp
from jax import lax
from jax.experimental import pallas as pl
from jax.experimental.pallas import tpu as pltpu
from jax.sharding import PartitionSpec as P

LN_EPS = 1e-5
ROPE_BASE = 10000.0
NEG_FILL = -1e30
MESH = pl.DeviceIdType.MESH
BLK = 256
HALF = 128
SIDES = range(2)
F32 = jnp.float32
BF16 = jnp.bfloat16


ORDER = (3, -3, 4, 2, -2, 1, -1, 0)


class Phases:
    def __init__(self):
        self.scope = None

    def __call__(self, name):
        if self.scope is not None:
            self.scope.__exit__(None, None, None)
        self.scope = jax.named_scope(name) if name else None
        if self.scope is not None:
            self.scope.__enter__()


def layer_kernel(chips, heads, x_hbm, gamma_hbm, beta_hbm, wqkv_hbm, wout_hbm, wup_hbm, wdown_hbm, k_hbm, v_hbm, pos_hbm,
                 inv_ref, out_ref, k_s, v_s,
                 x_s, gb_s, h_s, act_s, w_s, pos_s, lp_s, cs_s, sn_s, qk_s,
                 ps_s, pr_s, ss_s, ra_s, rb_s, ma_s, ost_s, orx_s, cz_s, ta_s, tb_s, tw_s, g_s, acc_s,
                 in_sem, up_sem, dn_sem, qkv_sem, kv_sem, wo_sem,
                 pd_send, pd_recv, qx_send, qx_recv, st_send, st_recv,
                 rs_send, rs_recv, aa_send, aa_recv, ma_send, ma_recv, mf_send, mf_recv, cg_send, cg_recv, cf_send, cf_recv):
    rows, d_model = x_hbm.shape
    ff = wup_hbm.shape[1]
    seq = k_hbm.shape[1]
    n_up = ff // BLK
    n_col = d_model // BLK
    half_heads = heads // 2
    slots = (heads + 2) // 2
    hr = rows // 2
    ml_at = 2 * hr
    chunk = 2 * hr + 8
    used = 2 * hr + 2
    top_rows = hr * half_heads
    up_rows, dn_rows = d_model, ff
    dn_base = n_up * up_rows
    qkv_base = dn_base + n_col * dn_rows
    n_kv = kv_sem.shape[1]
    kv_rows = rows // n_kv

    s = lax.axis_index('sp')
    z = lax.div(s, 2)
    c = lax.rem(s, 2)
    pc = 1 - c
    partner = {'sp': 2 * z + pc}

    def chip(k):
        return lax.rem(z + (k % chips), chips)

    def peer(k):
        return {'sp': 2 * chip(k) + c}

    def in_copy(i):
        src, dst = ((x_hbm, x_s), (gamma_hbm, gb_s.at[pl.ds(0, 1)]), (beta_hbm, gb_s.at[pl.ds(8, 1)]), (pos_hbm, pos_s))[i]
        return pltpu.make_async_copy(src, dst, in_sem.at[i])

    def up_copy(i):
        col = pl.multiple_of(i * BLK, BLK)
        row = pl.multiple_of(i * up_rows, BLK)
        return pltpu.make_async_copy(wup_hbm.at[:, pl.ds(col, BLK)], w_s.at[pl.ds(row, up_rows)], up_sem.at[i])

    def dn_copy(half, i):
        owner = pc if half == 0 else c
        col = pl.multiple_of((owner * chips + chip(ORDER[i])) * BLK, BLK)
        slot = half * chips + i
        row = pl.multiple_of(dn_base + slot * dn_rows, BLK)
        return pltpu.make_async_copy(wdown_hbm.at[:, pl.ds(col, BLK)], w_s.at[pl.ds(row, dn_rows)], dn_sem.at[slot])

    def qkv_copy(i):
        col = pl.multiple_of((c * slots + i) * BLK, BLK)
        row = pl.multiple_of(qkv_base + i * d_model, BLK)
        return pltpu.make_async_copy(wqkv_hbm.at[:, pl.ds(col, BLK)], w_s.at[pl.ds(row, d_model)], qkv_sem.at[i])

    def kv_copy(t, i):
        src, dst = ((k_hbm, k_s), (v_hbm, v_s))[t]
        sl = pl.ds(i * kv_rows, kv_rows)
        return pltpu.make_async_copy(src.at[sl], dst.at[sl], kv_sem.at[t, i])

    def wo_copy(i):
        col = pl.multiple_of(i * BLK, BLK)
        row = pl.multiple_of(i * d_model, BLK)
        return pltpu.make_async_copy(wout_hbm.at[:, pl.ds(col, BLK)], w_s.at[pl.ds(row, d_model)], wo_sem.at[i])

    def remote(src, dst, send, recv, to):
        return pltpu.make_async_remote_copy(src, dst, send, recv, device_id=to, device_id_type=MESH)

    def pd_copy(i):
        return remote(ps_s.at[i], pr_s.at[i], pd_send.at[i], pd_recv.at[i], partner)

    def qx_copy(owner, i):
        row = pl.multiple_of((owner * slots + i) * 2 * rows, 8)
        ref = qk_s.at[pl.ds(row, 2 * rows)]
        return remote(ref, ref, qx_send.at[i], qx_recv.at[i], partner)

    def st_copy(h):
        return remote(ost_s.at[pc, h], orx_s.at[h], st_send.at[h], st_recv.at[h], partner)

    def sign(side):
        return 1 - 2 * side

    def rows_of(side):
        return pl.ds(side * hr, hr)

    def rs_copy(kind, side):
        src = (ss_s.at[side], ss_s.at[2, rows_of(side)], ss_s.at[3 + side], ss_s.at[5 + side])[kind]
        dst = (ra_s.at[side], ra_s.at[2, rows_of(side)], rb_s.at[side], rb_s.at[2 + side])[kind]
        at = 2 * kind + side
        return remote(src, dst, rs_send.at[at], rs_recv.at[at], peer(sign(side) * (1 if kind in (0, 3) else 2)))

    def cz_at(h, k, n=chunk):
        return cz_s.at[pl.ds(pl.multiple_of((h * chips + chip(k)) * chunk, 8), n)]

    def aa_copy(h, kind, side):
        sg, rows_used = sign(side), pl.ds(0, used)
        src = tw_s.at[h, side, rows_used] if kind == 2 else cz_at(h, sg * (3, 4, 2, 1)[kind], used)
        dst = (ta_s.at[h, side], ta_s.at[h, 2], tb_s.at[h, side], tb_s.at[h, 2 + side])[kind].at[rows_used]
        at = 8 * h + 2 * kind + side
        return remote(src, dst, aa_send.at[at], aa_recv.at[at], peer(sg * (1 if kind in (0, 3) else 2)))

    def route(kind, side):
        return [sign(side) * v for v in ((0, 2), (0, 1), (-2, 1), (-2, 2))[kind]]

    def ma_part(kind, side, k, hop):
        ref = ma_s.at[c * chips + chip(k)]
        ref = ref.at[rows_of(side)] if kind == 3 else ref
        at = 2 * kind + side
        return remote(ref, ref, ma_send.at[at], ma_recv.at[at], peer(hop))

    def ma_copy(kind, side):
        return ma_part(kind, side, *route(kind, side))

    def ma_wait(kind, side):
        src, hop = route(kind, side)
        ma_part(kind, side, src - hop, hop).wait_recv()

    def cg_part(h, kind, side, k, hop):
        ref = g_s.at[c * chips + chip(k), rows_of(h)]
        at = 8 * h + 2 * kind + side
        return remote(ref, ref, cg_send.at[at], cg_recv.at[at], peer(hop))

    def cg_copy(h, kind, side):
        return cg_part(h, kind, side, *route(kind, side))

    def cg_wait(h, kind, side):
        src, hop = route(kind, side)
        cg_part(h, kind, side, src - hop, hop).wait_recv()

    def ma_fwd(owner, k):
        ref = ma_s.at[owner * chips + chip(k)]
        return remote(ref, ref, mf_send.at[k % chips], mf_recv.at[k % chips], partner)

    def cg_fwd(owner, k):
        ref = g_s.at[owner * chips + chip(k)]
        return remote(ref, ref, cf_send.at[k % chips], cf_recv.at[k % chips], partner)

    ph = Phases()
    ph('entry')
    for i in range(4):
        in_copy(i).start()
    for i in range(2):
        qkv_copy(i).start()
    bar = pltpu.get_barrier_semaphore()
    pl.semaphore_signal(bar, inc=1, device_id=partner, device_id_type=MESH)
    for k in (1, -1, 2, -2):
        pl.semaphore_signal(bar, inc=1, device_id=peer(k), device_id_type=MESH)

    ph('in_wait')
    for i in range(4):
        in_copy(i).wait()
    for i in range(2, 5):
        qkv_copy(i).start()
    ph('layer_norm')

    @pl.loop(0, rows // 16)
    def _(i):
        sl = pl.ds(pl.multiple_of(i * 16, 16), 16)
        xf = x_s[sl, :].astype(F32)
        mean = jnp.mean(xf, axis=-1, keepdims=True)
        cen = xf - mean
        var = jnp.mean(cen * cen, axis=-1, keepdims=True)
        h_s[sl, :] = (cen * lax.rsqrt(var + LN_EPS) * gb_s[0:1, :] + gb_s[8:9, :]).astype(BF16)

    qkv_copy(5).start()
    nil = jnp.zeros((half_heads, HALF), F32)
    for h in range(2):
        for i in range(used, chunk):
            cz_s[pl.ds(h * chips * chunk + i, half_heads, stride=chunk), :] = nil
    ph('rope')
    for b in range(rows):
        lp_s[b:b + 1, :] = jnp.full((1, HALF), pos_s[b], jnp.int32).astype(F32)
    ang = lp_s[...] * inv_ref[...]
    cs_s[...] = jnp.cos(ang)
    sn_s[...] = jnp.sin(ang)
    lp_s[...] = lp_s[...] - (s * seq).astype(F32)

    def chunk_dots(a_ref, bases, depth):
        accs = [None] * len(bases)
        for kk in range(depth // BLK):
            a = a_ref[:, kk * BLK:(kk + 1) * BLK]
            for j, row in enumerate(bases):
                w = w_s[pl.ds(pl.multiple_of(row + kk * BLK, BLK), BLK), :]
                p = jnp.dot(a, w, preferred_element_type=F32)
                accs[j] = p if accs[j] is None else accs[j] + p
        return accs

    def qkv_store(i, acc, send=True):
        a = acc.astype(BF16).astype(F32)
        a1, a2 = a[:, :HALF], a[:, HALF:]
        cs, sn = cs_s[...], sn_s[...]
        r1 = (a1 * cs - a2 * sn).astype(BF16).astype(F32)
        r2 = (a2 * cs + a1 * sn).astype(BF16).astype(F32)
        slot = c * slots + i
        is_v = slot == heads + 1
        row = pl.multiple_of(slot * 2 * rows, 8)
        qk_s[pl.ds(row, rows), :] = jnp.where(is_v, a1, r1)
        qk_s[pl.ds(row + rows, rows), :] = jnp.where(is_v, a2, r2)
        if send:
            qx_copy(c, i).start()

    def qkv_pair(i, send=True):
        qkv_copy(2 * i).wait()
        qkv_copy(2 * i + 1).wait()
        for j, acc in enumerate(chunk_dots(h_s, [qkv_base + (2 * i + j) * d_model for j in range(2)], d_model)):
            qkv_store(2 * i + j, acc, send)

    n_pair = slots // 2
    ph('qkv')
    qkv_pair(0, False)
    for i in range(6, slots):
        qkv_copy(i).start()
    ph('barrier')
    pl.semaphore_wait(bar, 5)
    ph('qkv2')
    for i in range(2):
        qx_copy(c, i).start()
    pl.loop(1, n_pair - 1)(qkv_pair)
    for i in range(n_kv):
        kv_copy(0, i).start()
        kv_copy(1, i).start()

    ph('qkv_last')
    qkv_pair(n_pair - 1)
    for i in range(2 * n_pair, slots):
        qkv_copy(i).wait()
        qkv_store(i, chunk_dots(h_s, [qkv_base + i * d_model], d_model)[0])

    ph('qkv_wait')
    for i in range(slots):
        qx_copy(pc, i).wait_recv()
    lane = lax.broadcasted_iota(jnp.int32, (heads, seq), 1)
    lane_f = lane.astype(F32)
    scale = k_s.shape[2] ** -0.5
    group = rows // 4

    def attend(h, g, carry):
        mm, ll = carry
        base = g * group
        kv_copy(0, g).wait()
        kv_copy(1, g).wait()
        scores, values, here = [], [], []
        for r in range(group):
            b = base + r

            def both(at, n):
                return jnp.concatenate([qk_s[pl.ds(at + b, n, stride=2 * rows), :], qk_s[pl.ds(at + rows + b, n, stride=2 * rows), :]], axis=-1)

            def one(at):
                return jnp.concatenate([qk_s[pl.ds(at + b, 1), :], qk_s[pl.ds(at + rows + b, 1), :]], axis=-1)

            q = both(0, heads)
            kn = one(2 * heads * rows)
            lp = lp_s[pl.ds(b, 1), :]
            here.append(lane_f == lp)
            sc = lax.dot_general(q.astype(BF16), k_s[b], (((1,), (1,)), ((), ())), preferred_element_type=F32)
            sc = jnp.where(here[r], jnp.sum(q * kn, axis=-1, keepdims=True), sc) * scale
            scores.append(jnp.where(lane_f <= lp, sc, NEG_FILL))
            values.append(one((2 * heads + 2) * rows))
        es, news = [], []
        for r in range(group):
            m = jnp.max(scores[r], axis=-1, keepdims=True)
            e = jnp.where(lane_f <= lp_s[pl.ds(base + r, 1), :], jnp.exp(scores[r] - m), 0.0)
            col = lane == base + r - h * hr
            mm = jnp.where(col, m, mm)
            ll = jnp.where(col, jnp.sum(e, axis=-1, keepdims=True), ll)
            eb = e.astype(BF16).astype(F32)
            news.append(jnp.sum(jnp.where(here[r], eb, 0.0), axis=-1, keepdims=True))
            es.append(jnp.where(here[r], 0.0, eb).astype(BF16))
        for r in range(group):
            b = base + r
            o = jnp.dot(es[r], v_s[b], preferred_element_type=F32) + news[r] * values[r]
            at = pl.ds(pl.multiple_of((b - h * hr) * half_heads, 8), half_heads)
            ost_s[0, h, at, :] = o[:half_heads]
            ost_s[1, h, at, :] = o[half_heads:]
        return mm, ll

    def attend_half(h):
        zero = jnp.zeros((heads, seq), F32)
        mm, ll = lax.fori_loop(2 * h, 2 * h + 2, functools.partial(attend, h), (zero, zero))
        ml = jnp.concatenate([mm, ll], axis=-1)
        ost_s[0, h, top_rows:, :] = ml[:half_heads]
        ost_s[1, h, top_rows:, :] = ml[half_heads:]
        st_copy(h).start()

    ph('attention')
    for i in range(n_up):
        up_copy(i).start()
    attend_half(0)

    ph('attention_last')
    attend_half(1)
    for half in range(2):
        for i in range(chips):
            dn_copy(half, i).start()

    def merge(h):
        m_s, l_s = ost_s[c, h, top_rows:, :HALF], ost_s[c, h, top_rows:, HALF:]
        m_p, l_p = orx_s[h, top_rows:, :HALF], orx_s[h, top_rows:, HALF:]
        m_c = jnp.maximum(m_s, m_p)
        w_own, w_par = jnp.exp(m_s - m_c), jnp.exp(m_p - m_c)

        def put(at, val):
            cz_s[pl.ds(h * chips * chunk + at, half_heads, stride=chunk), :] = val

        for b in range(hr):
            sl = slice(b * half_heads, (b + 1) * half_heads)
            mix = ost_s[c, h, sl, :] * w_own[:, b:b + 1] + orx_s[h, sl, :] * w_par[:, b:b + 1]
            put(b, mix[:, :HALF])
            put(hr + b, mix[:, HALF:])
        put(ml_at, m_c)
        put(ml_at + 1, l_s * w_own + l_p * w_par)

    def mlp_up(i):
        up_copy(i).wait()
        up_copy(i + 1).wait()
        us = chunk_dots(h_s, [(i + j) * up_rows for j in range(2)], up_rows)
        for j, u in enumerate(us):
            g = 0.5 * u * (1.0 + lax.erf(u * (0.5 ** 0.5)))
            act_s[:, (i + j) * BLK:(i + j + 1) * BLK] = g.astype(BF16)

    def blend(refs, out):
        ms = [ref[ml_at:ml_at + 1, :] for ref in refs]
        ls = [ref[ml_at + 1:ml_at + 2, :] for ref in refs]
        top = functools.reduce(jnp.maximum, ms)
        ws = [jnp.exp(m - top) for m in ms]
        l_sum = functools.reduce(lambda a, b: a + b, [l * w for l, w in zip(ls, ws)])
        pad = [jnp.zeros_like(top)] * (8 - len(refs) - 1)
        cols = jnp.transpose(jnp.concatenate(ws + [l_sum] + pad, axis=0))[:hr]
        for t in range(2):
            terms = [ref[t * hr:(t + 1) * hr, :] * cols[:, j:j + 1] for j, ref in enumerate(refs)]
            out(t, functools.reduce(lambda a, b: a + b, terms), cols[:, len(refs):len(refs) + 1])
        return top, l_sum

    slot_f = lax.broadcasted_iota(jnp.int32, (seq, HALF), 0).astype(F32)

    def insert(ref, head):
        @pl.loop(0, rows)
        def _(b):
            hit = slot_f == lp_s[pl.ds(b, 1), :]
            for t in range(2):
                new = qk_s[pl.ds((2 * head + t) * rows + b, 1), :]
                sl = slice(t * HALF, (t + 1) * HALF)
                ref[b, :, sl] = jnp.where(hit, new, ref[b, :, sl].astype(F32)).astype(BF16)

    for h in range(2):
        ph(f'stat_wait{h}')
        st_copy(h).wait_recv()
        ph(f'merge{h}')
        merge(h)
        aa_copy(h, 1, h).start()
        for side in SIDES:
            aa_copy(h, 0, side).start()
        ph(f'mlp_up{h}')
        if h == 1:
            for k in range(2):
                for side in SIDES:
                    aa_copy(k, 3, side).start()
            for i in range(n_col // 2, n_col):
                wo_copy(i).start()
        mlp_up(h * n_up // 2)
    ph('down_partner')
    for i in range(0, chips, 4):
        for j in range(4):
            dn_copy(0, i + j).wait()
        for j, p in enumerate(chunk_dots(act_s, [dn_base + (i + j) * dn_rows for j in range(4)], dn_rows)):
            ps_s[i + j] = p
            pd_copy(i + j).start()

    ph('down_own')
    for i in range(0, chips, 4):
        for j in range(4):
            dn_copy(1, i + j).wait()
        for j, p in enumerate(chunk_dots(act_s, [dn_base + (chips + i + j) * dn_rows for j in range(4)], dn_rows)):
            n = i + j
            pd_copy(n).wait_recv()
            ss_s[n] = p + pr_s[n]
            if n < 2:
                rs_copy(0, n).start()
            elif n == 2:
                for side in SIDES:
                    rs_copy(1, side).start()

    for side in SIDES:
        rs_copy(3, side).start()
    for i in range(n_col // 2):
        wo_copy(i).start()
    for h in range(2):
        ph(f'aa_wait{h}')
        aa_copy(h, 1, h).wait_recv()
        for side in SIDES:
            aa_copy(h, 0, side).wait_recv()
        ph(f'aa_add{h}')
        for side in range(2):
            def keep(t, acc, _):
                tw_s[h, side, t * hr:(t + 1) * hr, :] = acc

            more = [ta_s.at[h, 2]] if side == h else []
            top, l_sum = blend([cz_at(h, sign(side) * 2), ta_s.at[h, side]] + more, keep)
            tw_s[h, side, ml_at:, :] = jnp.concatenate([top, l_sum, jnp.zeros((6, HALF), F32)], axis=0)
            aa_copy(h, 2, side).start()
    ph('insert_k')
    insert(k_s, heads)
    ph('insert_v')
    insert(v_s, heads + 1)
    ph('rs_add')
    for side in SIDES:
        rs_copy(0, side).wait_recv()
        rs_copy(1, side).wait_recv()
        ss_s[3 + side] = ss_s[3 + side] + ra_s[side]
        ss_s[3 + side, rows_of(side)] = ss_s[3 + side, rows_of(side)] + ra_s[2, rows_of(side)]
        rs_copy(2, side).start()
    for h in range(2):
        ph(f'aa_last{h}')
        for side in SIDES:
            aa_copy(h, 2, side).wait_recv()
            aa_copy(h, 3, side).wait_recv()
        ph(f'context{h}')

        def finish(t, acc, l_col):
            g_s[c * chips + z, h * hr:(h + 1) * hr, t * HALF:(t + 1) * HALF] = (acc / l_col).astype(BF16).astype(F32)

        blend([cz_at(h, 0)] + [tb_s.at[h, j] for j in range(4)], finish)
        for kind in range(2):
            for side in SIDES:
                cg_copy(h, kind, side).start()
    cg_fwd(c, 0).start()
    ph('wo_wait')
    for i in range(n_col):
        wo_copy(i).wait()

    def out_dots(todo, first=False):
        lhs = [g_s[slot].astype(BF16) for slot in todo]
        for n in range(n_col):
            acc = None
            for slot, a in zip(todo, lhs):
                w = w_s[pl.ds(pl.multiple_of(n * d_model + slot * BLK, BLK), BLK), :]
                p = jnp.dot(a, w, preferred_element_type=F32)
                acc = p if acc is None else acc + p
            sl = slice(n * BLK, (n + 1) * BLK)
            acc_s[:, sl] = acc if first else acc_s[:, sl] + acc

    def mine(k):
        return c * chips + chip(k)

    def theirs(k):
        return pc * chips + chip(k)

    ph('out_0')
    out_dots([mine(0)], True)
    ph('cg_wait0')
    cg_fwd(pc, 0).wait_recv()
    ph('out_0b')
    out_dots([theirs(0)])
    ph('rs_sum')
    for side in SIDES:
        rs_copy(2, side).wait_recv()
        rs_copy(3, side).wait_recv()
    ma_s[c * chips + z] = ss_s[7] + rb_s[0] + rb_s[1] + rb_s[2] + rb_s[3]
    for kind in range(2):
        for side in SIDES:
            ma_copy(kind, side).start()
    ma_fwd(c, 0).start()

    ph('cg_wait1')
    for h in range(2):
        for side in SIDES:
            cg_wait(h, 0, side)
            if h == side:
                cg_copy(h, 3, side).start()
            cg_copy(h, 2, side).start()
    for k in (-2, 2):
        cg_fwd(c, k).start()
    for side in SIDES:
        for h in range(2):
            cg_wait(h, 1, side)
        cg_fwd(c, -sign(side)).start()
    ph('out_1')
    out_dots([mine(-2), mine(2), mine(-1), mine(1)])
    ph('ma_on')
    for side in SIDES:
        ma_wait(0, side)
        ma_copy(3, side).start()
        ma_copy(2, side).start()
        ma_fwd(c, -2 * sign(side)).start()
    for side in SIDES:
        ma_wait(1, side)
        ma_fwd(c, -sign(side)).start()

    ph('cg_wait2')
    for k in (-2, 2, -1, 1):
        cg_fwd(pc, k).wait_recv()
    ph('out_2')
    out_dots([theirs(-2), theirs(2), theirs(-1), theirs(1)])
    ph('cg_wait3')
    for side in SIDES:
        for h in range(2):
            cg_wait(h, 2, side)
        cg_fwd(c, -3 * sign(side)).start()
    ph('out_3')
    out_dots([mine(-3), mine(3)])
    ph('cg_wait4')
    for side in SIDES:
        cg_wait(side, 3, side)
    cg_fwd(c, 4).start()
    cg_fwd(pc, -3).wait_recv()
    cg_fwd(pc, 3).wait_recv()
    ph('out_4')
    out_dots([mine(4), theirs(-3), theirs(3)])
    ph('ma_tail')
    for side in SIDES:
        ma_wait(2, side)
        ma_wait(3, side)
        ma_fwd(c, -3 * sign(side)).start()
    ma_fwd(c, 4).start()
    ph('cg_wait5')
    cg_fwd(pc, 4).wait_recv()
    ph('out_5')
    out_dots([theirs(4)])
    ph('final')
    for k in range(chips):
        ma_fwd(pc, k).wait_recv()
    for n in range(n_col):
        sl = slice(n * BLK, (n + 1) * BLK)
        out_ref[:, sl] = (x_s[:, sl].astype(F32) + acc_s[:, sl] + ma_s[n]).astype(BF16)

    ph('drain')
    for i in range(chips):
        pd_copy(i).wait_send()
        ma_fwd(c, i).wait_send()
        cg_fwd(c, i).wait_send()
    for h in range(2):
        st_copy(h).wait_send()
    for kind in range(4):
        for side in SIDES:
            rs_copy(kind, side).wait_send()
            ma_copy(kind, side).wait_send()
            for h in range(2):
                if (h == side) or kind != 1:
                    aa_copy(h, kind, side).wait_send()
                if (h == side) or kind < 3:
                    cg_copy(h, kind, side).wait_send()
    for i in range(slots):
        qx_copy(c, i).wait_send()
    ph(None)


def store_kernel(*refs):
    srcs, dsts, sem = refs[:3], refs[3:6], refs[6]
    copies = []
    for n, (src, dst) in enumerate(zip(srcs, dsts)):
        parts = 1 if n == 0 else 4
        step = src.shape[0] // parts
        for i in range(parts):
            sl = pl.ds(i * step, step)
            copies.append(pltpu.make_async_copy(src.at[sl], dst.at[sl], sem.at[n, i]))
    for copy in copies:
        copy.start()
    for copy in copies:
        copy.wait()


def device_step(n_sp, hidden, ln_gamma, ln_beta, w_qkv, w_out, w_up, w_down, k_cache, v_cache, positions):
    rows, d_model = hidden.shape
    seq, head_dim = k_cache.shape[1], k_cache.shape[2]
    heads = w_out.shape[0] // head_dim
    ff = w_up.shape[1]
    chips = n_sp // 2
    slots = (heads + 2) // 2
    assert head_dim == BLK and heads == n_sp and d_model == n_sp * BLK and chips == 8
    inv_freq = 1.0 / (ROPE_BASE ** (jnp.arange(0, head_dim, 2, dtype=F32) / head_dim))
    n_up, n_col = ff // BLK, d_model // BLK
    w_rows = n_up * d_model + n_col * ff + slots * d_model
    n_kv = 4
    half = heads // 2
    any_spec = pl.BlockSpec(memory_space=pltpu.HBM)
    vmem_spec = pl.BlockSpec(memory_space=pltpu.VMEM)
    dma = pltpu.SemaphoreType.DMA
    hr = rows // 2
    chunk = 2 * hr + 8
    scratch = [
        pltpu.VMEM((rows, d_model), BF16),
        pltpu.VMEM((16, d_model), F32),
        pltpu.VMEM((rows, d_model), BF16),
        pltpu.VMEM((rows, ff), BF16),
        pltpu.VMEM((w_rows, BLK), BF16),
        pltpu.SMEM((rows,), jnp.int32),
        pltpu.VMEM((rows, HALF), F32),
        pltpu.VMEM((rows, HALF), F32),
        pltpu.VMEM((rows, HALF), F32),
        pltpu.VMEM(((heads + 2) * 2 * rows, HALF), F32),
        pltpu.VMEM((chips, rows, BLK), F32),
        pltpu.VMEM((chips, rows, BLK), F32),
        pltpu.VMEM((chips, rows, BLK), F32),
        pltpu.VMEM((3, rows, BLK), F32),
        pltpu.VMEM((4, rows, BLK), F32),
        pltpu.VMEM((n_sp, rows, BLK), F32),
        pltpu.VMEM((2, 2, (hr + 1) * half, BLK), F32),
        pltpu.VMEM((2, (hr + 1) * half, BLK), F32),
        pltpu.VMEM((2 * chips * chunk, HALF), F32),
        pltpu.VMEM((2, 3, chunk, HALF), F32),
        pltpu.VMEM((2, 4, chunk, HALF), F32),
        pltpu.VMEM((2, 2, chunk, HALF), F32),
        pltpu.VMEM((n_sp, rows, BLK), F32),
        pltpu.VMEM((rows, d_model), F32),
        dma((4,)), dma((n_up,)), dma((n_col,)), dma((slots,)), dma((2, n_kv)), dma((n_col,)),
        dma((chips,)), dma((chips,)), dma((slots,)), dma((slots,)), dma((2,)), dma((2,)),
    ] + [dma((n_sp,))] * 12
    in_hbm = [pltpu.with_memory_space_constraint(a, pltpu.HBM) for a in (hidden, ln_gamma.reshape(1, -1), ln_beta.reshape(1, -1))]
    results = pl.pallas_call(
        functools.partial(layer_kernel, chips, heads),
        out_shape=(pltpu.VMEM(hidden.shape, BF16), pltpu.VMEM(k_cache.shape, BF16), pltpu.VMEM(v_cache.shape, BF16)),
        in_specs=[any_spec] * 10 + [vmem_spec],
        out_specs=(vmem_spec, vmem_spec, vmem_spec),
        scratch_shapes=scratch,
        compiler_params=pltpu.CompilerParams(collective_id=0, has_side_effects=True, vmem_limit_bytes=46 * 1024 * 1024),
        name='decode_layer',
    )(*in_hbm, w_qkv, w_out, w_up, w_down, k_cache, v_cache, pltpu.with_memory_space_constraint(positions, pltpu.HBM), inv_freq.reshape(1, -1))
    return pl.pallas_call(
        store_kernel,
        out_shape=[jax.ShapeDtypeStruct(r.shape, r.dtype) for r in results],
        in_specs=[vmem_spec] * 3,
        out_specs=[pl.BlockSpec(memory_space=pltpu.HBM)] * 3,
        scratch_shapes=[dma((3, 4))],
        compiler_params=pltpu.CompilerParams(vmem_limit_bytes=1024 * 1024),
        name='store_results',
    )(*results)


def solution(mesh):
    rows, cache = P('dp'), P('dp', 'sp')
    in_specs = (rows, P(), P(), P(), P(), P(None, 'sp'), P('sp'), cache, cache, rows)
    out_specs = (rows, cache, cache)
    return jax.shard_map(functools.partial(device_step, mesh.shape['sp']), mesh=mesh, in_specs=in_specs, out_specs=out_specs, check_vma=False)
```

```python
import functools

import jax
import jax.numpy as jnp
from jax import lax
from jax.experimental import pallas as pl
from jax.experimental.pallas import tpu as pltpu
from jax.sharding import PartitionSpec as P

LN_EPS = 1e-5
ROPE_BASE = 10000.0
NEG_FILL = -1e30
MESH = pl.DeviceIdType.MESH
BLK = 256
HALF = 128
F32 = jnp.float32
BF16 = jnp.bfloat16


ORDER = (3, -3, 4, 2, -2, 1, -1, 0)


class Phases:
    def __init__(self):
        self.scope = None

    def __call__(self, name):
        if self.scope is not None:
            self.scope.__exit__(None, None, None)
        self.scope = jax.named_scope(name) if name else None
        if self.scope is not None:
            self.scope.__enter__()


def layer_kernel(chips, heads, x_hbm, gamma_hbm, beta_hbm, wqkv_hbm, wout_hbm, wup_hbm, wdown_hbm, k_hbm, v_hbm, pos_hbm,
                 inv_ref, out_ref, k_s, v_s,
                 x_s, gb_s, h_s, act_s, w_s, pos_s, lp_s, cs_s, sn_s, qk_s,
                 ps_s, pr_s, ss_s, ra_s, rb_s, ma_s, ost_s, orx_s, cz_s, ta_s, tb_s, tw_s, g_s, acc_s,
                 in_sem, up_sem, dn_sem, qkv_sem, kv_sem, wo_sem,
                 pd_send, pd_recv, qx_send, qx_recv, st_send, st_recv,
                 rs_send, rs_recv, aa_send, aa_recv, ma_send, ma_recv, mf_send, mf_recv, cg_send, cg_recv, cf_send, cf_recv):
    rows, d_model = x_hbm.shape
    ff = wup_hbm.shape[1]
    seq = k_hbm.shape[1]
    n_up = ff // BLK
    n_col = d_model // BLK
    half_heads = heads // 2
    slots = (heads + 2) // 2
    hr = rows // 2
    ml_at = 2 * hr
    chunk = 2 * hr + 8
    top_rows = hr * half_heads
    up_rows, dn_rows = d_model, ff
    dn_base = n_up * up_rows
    qkv_base = dn_base + n_col * dn_rows
    n_kv = kv_sem.shape[1]
    kv_rows = rows // n_kv

    s = lax.axis_index('sp')
    z = lax.div(s, 2)
    c = lax.rem(s, 2)
    pc = 1 - c
    partner = {'sp': 2 * z + pc}

    def chip(k):
        return lax.rem(z + (k % chips), chips)

    def peer(k):
        return {'sp': 2 * chip(k) + c}

    def in_copy(i):
        src, dst = ((x_hbm, x_s), (gamma_hbm, gb_s.at[pl.ds(0, 1)]), (beta_hbm, gb_s.at[pl.ds(8, 1)]), (pos_hbm, pos_s))[i]
        return pltpu.make_async_copy(src, dst, in_sem.at[i])

    def up_copy(i):
        col = pl.multiple_of(i * BLK, BLK)
        row = pl.multiple_of(i * up_rows, BLK)
        return pltpu.make_async_copy(wup_hbm.at[:, pl.ds(col, BLK)], w_s.at[pl.ds(row, up_rows)], up_sem.at[i])

    def dn_copy(half, i):
        owner = pc if half == 0 else c
        col = pl.multiple_of((owner * chips + chip(ORDER[i])) * BLK, BLK)
        slot = half * chips + i
        row = pl.multiple_of(dn_base + slot * dn_rows, BLK)
        return pltpu.make_async_copy(wdown_hbm.at[:, pl.ds(col, BLK)], w_s.at[pl.ds(row, dn_rows)], dn_sem.at[slot])

    def qkv_copy(i):
        col = pl.multiple_of((c * slots + i) * BLK, BLK)
        row = pl.multiple_of(qkv_base + i * d_model, BLK)
        return pltpu.make_async_copy(wqkv_hbm.at[:, pl.ds(col, BLK)], w_s.at[pl.ds(row, d_model)], qkv_sem.at[i])

    def kv_copy(t, i):
        src, dst = ((k_hbm, k_s), (v_hbm, v_s))[t]
        sl = pl.ds(i * kv_rows, kv_rows)
        return pltpu.make_async_copy(src.at[sl], dst.at[sl], kv_sem.at[t, i])

    def wo_copy(i):
        col = pl.multiple_of(i * BLK, BLK)
        row = pl.multiple_of(i * d_model, BLK)
        return pltpu.make_async_copy(wout_hbm.at[:, pl.ds(col, BLK)], w_s.at[pl.ds(row, d_model)], wo_sem.at[i])

    def remote(src, dst, send, recv, to):
        return pltpu.make_async_remote_copy(src, dst, send, recv, device_id=to, device_id_type=MESH)

    def pd_copy(i):
        return remote(ps_s.at[i], pr_s.at[i], pd_send.at[i], pd_recv.at[i], partner)

    def qx_copy(owner, i):
        row = pl.multiple_of((owner * slots + i) * 2 * rows, 8)
        ref = qk_s.at[pl.ds(row, 2 * rows)]
        return remote(ref, ref, qx_send.at[i], qx_recv.at[i], partner)

    def st_copy(h):
        return remote(ost_s.at[pc, h], orx_s.at[h], st_send.at[h], st_recv.at[h], partner)

    hops = (1, -1, 2, -2, 2, -2, 1, -1)

    def rs_copy(i):
        src = (ss_s.at[0], ss_s.at[1], ss_s.at[2, pl.ds(0, hr)], ss_s.at[2, pl.ds(hr, hr)], ss_s.at[3], ss_s.at[4], ss_s.at[5], ss_s.at[6])[i]
        dst = (ra_s.at[0], ra_s.at[1], ra_s.at[2, pl.ds(0, hr)], ra_s.at[2, pl.ds(hr, hr)], rb_s.at[0], rb_s.at[1], rb_s.at[2], rb_s.at[3])[i]
        return remote(src, dst, rs_send.at[i], rs_recv.at[i], peer(hops[i]))

    def cz_at(h, k):
        return cz_s.at[pl.ds(pl.multiple_of((h * chips + chip(k)) * chunk, 8), chunk)]

    def aa_copy(h, i):
        src = (lambda: cz_at(h, 3), lambda: cz_at(h, -3), lambda: cz_at(h, 4), lambda: tw_s.at[h, 0], lambda: tw_s.at[h, 1],
               lambda: cz_at(h, 1), lambda: cz_at(h, -1))[i]()
        dst = ta_s.at[h, i] if i < 3 else tb_s.at[h, i - 3]
        hop = (1, -1, (2, -2)[h], 2, -2, 1, -1)[i]
        return remote(src, dst, aa_send.at[7 * h + i], aa_recv.at[7 * h + i], peer(hop))

    g_hop = (2, -2, 1, -1, 1, -1, 2, -2)
    g_src = (0, 0, 0, 0, -2, 2, -2, 2)

    def gather_copy(buf, send, recv, i):
        ref = buf.at[c * chips + chip(g_src[i])]
        if i >= 6:
            ref = ref.at[pl.ds((i - 6) * hr, hr)]
        return remote(ref, ref, send.at[i], recv.at[i], peer(g_hop[i]))

    def gather_recv(buf, send, recv, i):
        ref = buf.at[c * chips + chip(g_src[i] - g_hop[i])]
        if i >= 6:
            ref = ref.at[pl.ds((i - 6) * hr, hr)]
        return remote(ref, ref, send.at[i], recv.at[i], peer(g_hop[i]))

    def ma_copy(i):
        return gather_copy(ma_s, ma_send, ma_recv, i)

    def cg_route(h, i):
        return ((0, 2), (0, -2), (0, 1), (0, -1), (-2, 1), (2, -1), ((-2, 2), (2, -2))[h])[i]

    def cg_part(h, i, k, hop):
        ref = g_s.at[c * chips + chip(k), pl.ds(h * hr, hr)]
        return remote(ref, ref, cg_send.at[7 * h + i], cg_recv.at[7 * h + i], peer(hop))

    def cg_copy(h, i):
        src, hop = cg_route(h, i)
        return cg_part(h, i, src, hop)

    def ma_wait(i):
        gather_recv(ma_s, ma_send, ma_recv, i).wait_recv()

    def cg_wait(h, i):
        src, hop = cg_route(h, i)
        cg_part(h, i, src - hop, hop).wait_recv()

    def ma_fwd(owner, k):
        ref = ma_s.at[owner * chips + chip(k)]
        return remote(ref, ref, mf_send.at[k % chips], mf_recv.at[k % chips], partner)

    def cg_fwd(owner, k):
        ref = g_s.at[owner * chips + chip(k)]
        return remote(ref, ref, cf_send.at[k % chips], cf_recv.at[k % chips], partner)

    ph = Phases()
    ph('entry')
    inputs = range(4)
    for i in inputs:
        in_copy(i).start()
    for i in range(2):
        qkv_copy(i).start()
    bar = pltpu.get_barrier_semaphore()
    pl.semaphore_signal(bar, inc=1, device_id=partner, device_id_type=MESH)
    for k in (1, -1, 2, -2):
        pl.semaphore_signal(bar, inc=1, device_id=peer(k), device_id_type=MESH)

    ph('in_wait')
    for i in inputs:
        in_copy(i).wait()
    for i in range(2, slots):
        qkv_copy(i).start()
    ph('layer_norm')

    @pl.loop(0, rows // 16)
    def _(i):
        sl = pl.ds(pl.multiple_of(i * 16, 16), 16)
        xf = x_s[sl, :].astype(F32)
        mean = jnp.mean(xf, axis=-1, keepdims=True)
        cen = xf - mean
        var = jnp.mean(cen * cen, axis=-1, keepdims=True)
        h_s[sl, :] = (cen * lax.rsqrt(var + LN_EPS) * gb_s[0:1, :] + gb_s[8:9, :]).astype(BF16)

    nil = jnp.zeros((half_heads, HALF), F32)
    for h in range(2):
        for i in range(ml_at + 2, chunk):
            cz_s[pl.ds(h * chips * chunk + i, half_heads, stride=chunk), :] = nil
    ph('rope')
    for b in range(rows):
        lp_s[b:b + 1, :] = jnp.full((1, HALF), pos_s[b], jnp.int32).astype(F32)
    ang = lp_s[...] * inv_ref[...]
    cs_s[...] = jnp.cos(ang)
    sn_s[...] = jnp.sin(ang)
    lp_s[...] = lp_s[...] - (s * seq).astype(F32)

    def chunk_dots(a_ref, bases, depth):
        accs = [None] * len(bases)
        for kk in range(depth // BLK):
            a = a_ref[:, kk * BLK:(kk + 1) * BLK]
            for j, row in enumerate(bases):
                w = w_s[pl.ds(pl.multiple_of(row + kk * BLK, BLK), BLK), :]
                p = jnp.dot(a, w, preferred_element_type=F32)
                accs[j] = p if accs[j] is None else accs[j] + p
        return accs

    def qkv_store(i, acc, send=True):
        a = acc.astype(BF16).astype(F32)
        a1, a2 = a[:, :HALF], a[:, HALF:]
        cs, sn = cs_s[...], sn_s[...]
        r1 = (a1 * cs - a2 * sn).astype(BF16).astype(F32)
        r2 = (a2 * cs + a1 * sn).astype(BF16).astype(F32)
        slot = c * slots + i
        is_v = slot == heads + 1
        row = pl.multiple_of(slot * 2 * rows, 8)
        qk_s[pl.ds(row, rows), :] = jnp.where(is_v, a1, r1)
        qk_s[pl.ds(row + rows, rows), :] = jnp.where(is_v, a2, r2)
        if send:
            qx_copy(c, i).start()

    def qkv_pair(i, send=True):
        qkv_copy(2 * i).wait()
        qkv_copy(2 * i + 1).wait()
        for j, acc in enumerate(chunk_dots(h_s, [qkv_base + (2 * i + j) * d_model for j in range(2)], d_model)):
            qkv_store(2 * i + j, acc, send)

    n_pair = slots // 2
    ph('qkv')
    qkv_pair(0, False)
    ph('barrier')
    pl.semaphore_wait(bar, 5)
    ph('qkv2')
    for i in range(2):
        qx_copy(c, i).start()
    pl.loop(1, n_pair - 1)(qkv_pair)
    for i in range(n_kv):
        kv_copy(0, i).start()
        kv_copy(1, i).start()

    ph('qkv_last')
    qkv_pair(n_pair - 1)
    for i in range(2 * n_pair, slots):
        qkv_copy(i).wait()
        qkv_store(i, chunk_dots(h_s, [qkv_base + i * d_model], d_model)[0])

    ph('qkv_wait')
    for i in range(slots):
        qx_copy(pc, i).wait_recv()
    lane = lax.broadcasted_iota(jnp.int32, (heads, seq), 1)
    lane_f = lane.astype(F32)
    scale = k_s.shape[2] ** -0.5
    group = rows // 4

    def attend(h, g, carry):
        mm, ll = carry
        base = g * group
        kv_copy(0, g).wait()
        kv_copy(1, g).wait()
        scores, values, here = [], [], []
        for r in range(group):
            b = base + r

            def both(at, n):
                return jnp.concatenate([qk_s[pl.ds(at + b, n, stride=2 * rows), :], qk_s[pl.ds(at + rows + b, n, stride=2 * rows), :]], axis=-1)

            def one(at):
                return jnp.concatenate([qk_s[pl.ds(at + b, 1), :], qk_s[pl.ds(at + rows + b, 1), :]], axis=-1)

            q = both(0, heads)
            kn = one(2 * heads * rows)
            lp = lp_s[pl.ds(b, 1), :]
            here.append(lane_f == lp)
            sc = lax.dot_general(q.astype(BF16), k_s[b], (((1,), (1,)), ((), ())), preferred_element_type=F32)
            sc = jnp.where(here[r], jnp.sum(q * kn, axis=-1, keepdims=True), sc) * scale
            scores.append(jnp.where(lane_f <= lp, sc, NEG_FILL))
            values.append(one((2 * heads + 2) * rows))
        es, news = [], []
        for r in range(group):
            m = jnp.max(scores[r], axis=-1, keepdims=True)
            e = jnp.where(lane_f <= lp_s[pl.ds(base + r, 1), :], jnp.exp(scores[r] - m), 0.0)
            col = lane == base + r - h * hr
            mm = jnp.where(col, m, mm)
            ll = jnp.where(col, jnp.sum(e, axis=-1, keepdims=True), ll)
            eb = e.astype(BF16).astype(F32)
            news.append(jnp.sum(jnp.where(here[r], eb, 0.0), axis=-1, keepdims=True))
            es.append(jnp.where(here[r], 0.0, eb).astype(BF16))
        for r in range(group):
            b = base + r
            o = jnp.dot(es[r], v_s[b], preferred_element_type=F32) + news[r] * values[r]
            at = pl.ds(pl.multiple_of((b - h * hr) * half_heads, 8), half_heads)
            ost_s[0, h, at, :] = o[:half_heads]
            ost_s[1, h, at, :] = o[half_heads:]
        return mm, ll

    def attend_half(h):
        zero = jnp.zeros((heads, seq), F32)
        mm, ll = lax.fori_loop(2 * h, 2 * h + 2, functools.partial(attend, h), (zero, zero))
        ml = jnp.concatenate([mm, ll], axis=-1)
        ost_s[0, h, top_rows:, :] = ml[:half_heads]
        ost_s[1, h, top_rows:, :] = ml[half_heads:]
        st_copy(h).start()

    ph('attention')
    for i in range(n_up):
        up_copy(i).start()
    attend_half(0)

    ph('attention_last')
    attend_half(1)
    for half in range(2):
        for i in range(chips):
            dn_copy(half, i).start()

    def merge(h):
        m_s, l_s = ost_s[c, h, top_rows:, :HALF], ost_s[c, h, top_rows:, HALF:]
        m_p, l_p = orx_s[h, top_rows:, :HALF], orx_s[h, top_rows:, HALF:]
        m_c = jnp.maximum(m_s, m_p)
        w_own, w_par = jnp.exp(m_s - m_c), jnp.exp(m_p - m_c)

        def put(at, val):
            cz_s[pl.ds(h * chips * chunk + at, half_heads, stride=chunk), :] = val

        for b in range(hr):
            sl = slice(b * half_heads, (b + 1) * half_heads)
            mix = ost_s[c, h, sl, :] * w_own[:, b:b + 1] + orx_s[h, sl, :] * w_par[:, b:b + 1]
            put(b, mix[:, :HALF])
            put(hr + b, mix[:, HALF:])
        put(ml_at, m_c)
        put(ml_at + 1, l_s * w_own + l_p * w_par)

    def mlp_up(i):
        up_copy(i).wait()
        up_copy(i + 1).wait()
        us = chunk_dots(h_s, [(i + j) * up_rows for j in range(2)], up_rows)
        for j, u in enumerate(us):
            g = 0.5 * u * (1.0 + lax.erf(u * (0.5 ** 0.5)))
            act_s[:, (i + j) * BLK:(i + j + 1) * BLK] = g.astype(BF16)

    def blend(refs, out):
        ms = [ref[ml_at:ml_at + 1, :] for ref in refs]
        ls = [ref[ml_at + 1:ml_at + 2, :] for ref in refs]
        top = functools.reduce(jnp.maximum, ms)
        ws = [jnp.exp(m - top) for m in ms]
        l_sum = functools.reduce(lambda a, b: a + b, [l * w for l, w in zip(ls, ws)])
        pad = [jnp.zeros_like(top)] * (8 - len(refs) - 1)
        cols = jnp.transpose(jnp.concatenate(ws + [l_sum] + pad, axis=0))[:hr]
        for t in range(2):
            terms = [ref[t * hr:(t + 1) * hr, :] * cols[:, j:j + 1] for j, ref in enumerate(refs)]
            out(t, functools.reduce(lambda a, b: a + b, terms), cols[:, len(refs):len(refs) + 1])
        return top, l_sum

    slot_f = lax.broadcasted_iota(jnp.int32, (seq, HALF), 0).astype(F32)

    def insert(ref, head):
        @pl.loop(0, rows)
        def _(b):
            hit = slot_f == lp_s[pl.ds(b, 1), :]
            for t in range(2):
                new = qk_s[pl.ds((2 * head + t) * rows + b, 1), :]
                sl = slice(t * HALF, (t + 1) * HALF)
                ref[b, :, sl] = jnp.where(hit, new, ref[b, :, sl].astype(F32)).astype(BF16)

    for h in range(2):
        ph(f'stat_wait{h}')
        st_copy(h).wait_recv()
        ph(f'merge{h}')
        merge(h)
        for i in (2, 0, 1):
            aa_copy(h, i).start()
        ph(f'mlp_up{h}')
        if h == 1:
            for k in range(2):
                for i in (5, 6):
                    aa_copy(k, i).start()
            for i in range(n_col // 2, n_col):
                wo_copy(i).start()
        mlp_up(h * n_up // 2)
    ph('down_partner')
    for i in range(0, chips, 4):
        for j in range(4):
            dn_copy(0, i + j).wait()
        for j, p in enumerate(chunk_dots(act_s, [dn_base + (i + j) * dn_rows for j in range(4)], dn_rows)):
            ps_s[i + j] = p
            pd_copy(i + j).start()

    ph('down_own')
    for i in range(0, chips, 4):
        for j in range(4):
            dn_copy(1, i + j).wait()
        for j, p in enumerate(chunk_dots(act_s, [dn_base + (chips + i + j) * dn_rows for j in range(4)], dn_rows)):
            n = i + j
            pd_copy(n).wait_recv()
            ss_s[n] = p + pr_s[n]
            for m in ((0,), (1,), (2, 3), (), (), (6,), (7,), ())[n]:
                rs_copy(m).start()

    for i in range(n_col // 2):
        wo_copy(i).start()
    for h in range(2):
        ph(f'aa_wait{h}')
        for i in range(3):
            aa_copy(h, i).wait_recv()
        ph(f'aa_add{h}')
        for side in range(2):
            def keep(t, acc, _):
                tw_s[h, side, t * hr:(t + 1) * hr, :] = acc

            more = [ta_s.at[h, 2]] if side == h else []
            top, l_sum = blend([cz_at(h, (2, -2)[side]), ta_s.at[h, side]] + more, keep)
            tw_s[h, side, ml_at:, :] = jnp.concatenate([top, l_sum, jnp.zeros((6, HALF), F32)], axis=0)
            aa_copy(h, 3 + side).start()
    ph('insert_k')
    insert(k_s, heads)
    ph('rs_add')
    for i in range(4):
        rs_copy(i).wait_recv()
    ss_s[3, 0:hr] = ss_s[3, 0:hr] + ra_s[0, 0:hr] + ra_s[2, 0:hr]
    ss_s[3, hr:] = ss_s[3, hr:] + ra_s[0, hr:]
    ss_s[4, 0:hr] = ss_s[4, 0:hr] + ra_s[1, 0:hr]
    ss_s[4, hr:] = ss_s[4, hr:] + ra_s[1, hr:] + ra_s[2, hr:]
    rs_copy(4).start()
    rs_copy(5).start()
    ph('insert_v')
    insert(v_s, heads + 1)
    for h in range(2):
        ph(f'aa_last{h}')
        for i in range(3, 7):
            aa_copy(h, i).wait_recv()
        ph(f'context{h}')

        def finish(t, acc, l_col):
            g_s[c * chips + z, h * hr:(h + 1) * hr, t * HALF:(t + 1) * HALF] = (acc / l_col).astype(BF16).astype(F32)

        blend([cz_at(h, 0)] + [tb_s.at[h, j] for j in range(4)], finish)
        for i in range(4):
            cg_copy(h, i).start()
    cg_fwd(c, 0).start()

    ph('rs_sum')
    for i in range(4, 8):
        rs_copy(i).wait_recv()
    ma_s[c * chips + z] = ss_s[7] + rb_s[0] + rb_s[1] + rb_s[2] + rb_s[3]
    for i in range(4):
        ma_copy(i).start()
    ma_fwd(c, 0).start()

    ph('wo_wait')
    for i in range(n_col):
        wo_copy(i).wait()

    def out_dots(todo, first=False):
        lhs = [g_s[slot].astype(BF16) for slot in todo]
        for n in range(n_col):
            acc = None
            for slot, a in zip(todo, lhs):
                w = w_s[pl.ds(pl.multiple_of(n * d_model + slot * BLK, BLK), BLK), :]
                p = jnp.dot(a, w, preferred_element_type=F32)
                acc = p if acc is None else acc + p
            sl = slice(n * BLK, (n + 1) * BLK)
            acc_s[:, sl] = acc if first else acc_s[:, sl] + acc

    def mine(k):
        return c * chips + chip(k)

    def theirs(k):
        return pc * chips + chip(k)

    ph('out_0')
    out_dots([mine(0)], True)
    ph('cg_wait0')
    cg_fwd(pc, 0).wait_recv()
    ph('out_0b')
    out_dots([theirs(0)])
    ph('cg_wait1')
    for h in range(2):
        cg_wait(h, 0)
        if h == 0:
            cg_copy(0, 6).start()
        cg_copy(h, 4).start()
        cg_wait(h, 1)
        if h == 1:
            cg_copy(1, 6).start()
        cg_copy(h, 5).start()
    cg_fwd(c, -2).start()
    cg_fwd(c, 2).start()
    cg_wait(0, 2)
    cg_wait(1, 2)
    cg_fwd(c, -1).start()
    cg_wait(0, 3)
    cg_wait(1, 3)
    cg_fwd(c, 1).start()
    ph('out_1')
    out_dots([mine(-2), mine(2), mine(-1), mine(1)])
    ph('ma_on')
    ma_wait(0)
    ma_wait(1)
    for i in range(4, 8):
        ma_copy(i).start()
    ma_wait(2)
    ma_wait(3)
    for k in (2, -2, 1, -1):
        ma_fwd(c, k).start()

    ph('cg_wait2')
    for k in (-2, 2, -1, 1):
        cg_fwd(pc, k).wait_recv()
    ph('out_2')
    out_dots([theirs(-2), theirs(2), theirs(-1), theirs(1)])
    ph('cg_wait3')
    cg_wait(0, 4)
    cg_wait(1, 4)
    cg_fwd(c, -3).start()
    cg_wait(0, 5)
    cg_wait(1, 5)
    cg_fwd(c, 3).start()
    ph('out_3')
    out_dots([mine(-3), mine(3)])
    ph('cg_wait4')
    cg_wait(0, 6)
    cg_wait(1, 6)
    cg_fwd(c, 4).start()
    cg_fwd(pc, -3).wait_recv()
    cg_fwd(pc, 3).wait_recv()
    ph('out_4')
    out_dots([mine(4), theirs(-3), theirs(3)])
    ph('ma_tail')
    for i in range(4, 8):
        ma_wait(i)
    for k in (3, -3, 4):
        ma_fwd(c, k).start()
    ph('cg_wait5')
    cg_fwd(pc, 4).wait_recv()
    ph('out_5')
    out_dots([theirs(4)])
    ph('final')
    for k in range(chips):
        ma_fwd(pc, k).wait_recv()
    for n in range(n_col):
        sl = slice(n * BLK, (n + 1) * BLK)
        out_ref[:, sl] = (x_s[:, sl].astype(F32) + acc_s[:, sl] + ma_s[n]).astype(BF16)

    ph('drain')
    for i in range(chips):
        pd_copy(i).wait_send()
        ma_fwd(c, i).wait_send()
        cg_fwd(c, i).wait_send()
    for i in range(8):
        rs_copy(i).wait_send()
        ma_copy(i).wait_send()
    for h in range(2):
        st_copy(h).wait_send()
        for i in range(7):
            aa_copy(h, i).wait_send()
            cg_copy(h, i).wait_send()
    for i in range(slots):
        qx_copy(c, i).wait_send()
    ph(None)


def store_kernel(*refs):
    srcs, dsts, sem = refs[:3], refs[3:6], refs[6]
    copies = []
    for n, (src, dst) in enumerate(zip(srcs, dsts)):
        parts = 1 if n == 0 else 4
        step = src.shape[0] // parts
        for i in range(parts):
            sl = pl.ds(i * step, step)
            copies.append(pltpu.make_async_copy(src.at[sl], dst.at[sl], sem.at[n, i]))
    for copy in copies:
        copy.start()
    for copy in copies:
        copy.wait()


def device_step(n_sp, hidden, ln_gamma, ln_beta, w_qkv, w_out, w_up, w_down, k_cache, v_cache, positions):
    rows, d_model = hidden.shape
    seq, head_dim = k_cache.shape[1], k_cache.shape[2]
    heads = w_out.shape[0] // head_dim
    ff = w_up.shape[1]
    chips = n_sp // 2
    slots = (heads + 2) // 2
    assert head_dim == BLK and heads == n_sp and d_model == n_sp * BLK and chips == 8
    inv_freq = 1.0 / (ROPE_BASE ** (jnp.arange(0, head_dim, 2, dtype=F32) / head_dim))
    n_up, n_col = ff // BLK, d_model // BLK
    w_rows = n_up * d_model + n_col * ff + slots * d_model
    n_kv = 4
    half = heads // 2
    any_spec = pl.BlockSpec(memory_space=pltpu.HBM)
    vmem_spec = pl.BlockSpec(memory_space=pltpu.VMEM)
    dma = pltpu.SemaphoreType.DMA
    hr = rows // 2
    chunk = 2 * hr + 8
    scratch = [
        pltpu.VMEM((rows, d_model), BF16),
        pltpu.VMEM((16, d_model), F32),
        pltpu.VMEM((rows, d_model), BF16),
        pltpu.VMEM((rows, ff), BF16),
        pltpu.VMEM((w_rows, BLK), BF16),
        pltpu.SMEM((rows,), jnp.int32),
        pltpu.VMEM((rows, HALF), F32),
        pltpu.VMEM((rows, HALF), F32),
        pltpu.VMEM((rows, HALF), F32),
        pltpu.VMEM(((heads + 2) * 2 * rows, HALF), F32),
        pltpu.VMEM((chips, rows, BLK), F32),
        pltpu.VMEM((chips, rows, BLK), F32),
        pltpu.VMEM((chips, rows, BLK), F32),
        pltpu.VMEM((3, rows, BLK), F32),
        pltpu.VMEM((4, rows, BLK), F32),
        pltpu.VMEM((n_sp, rows, BLK), F32),
        pltpu.VMEM((2, 2, (hr + 1) * half, BLK), F32),
        pltpu.VMEM((2, (hr + 1) * half, BLK), F32),
        pltpu.VMEM((2 * chips * chunk, HALF), F32),
        pltpu.VMEM((2, 3, chunk, HALF), F32),
        pltpu.VMEM((2, 4, chunk, HALF), F32),
        pltpu.VMEM((2, 2, chunk, HALF), F32),
        pltpu.VMEM((n_sp, rows, BLK), F32),
        pltpu.VMEM((rows, d_model), F32),
        dma((4,)), dma((n_up,)), dma((n_col,)), dma((slots,)), dma((2, n_kv)), dma((n_col,)),
        dma((chips,)), dma((chips,)), dma((slots,)), dma((slots,)), dma((2,)), dma((2,)),
    ] + [dma((n_sp,))] * 12
    in_hbm = [pltpu.with_memory_space_constraint(a, pltpu.HBM) for a in (hidden, ln_gamma.reshape(1, -1), ln_beta.reshape(1, -1))]
    results = pl.pallas_call(
        functools.partial(layer_kernel, chips, heads),
        out_shape=(pltpu.VMEM(hidden.shape, BF16), pltpu.VMEM(k_cache.shape, BF16), pltpu.VMEM(v_cache.shape, BF16)),
        in_specs=[any_spec] * 10 + [vmem_spec],
        out_specs=(vmem_spec, vmem_spec, vmem_spec),
        scratch_shapes=scratch,
        compiler_params=pltpu.CompilerParams(collective_id=0, has_side_effects=True, vmem_limit_bytes=46 * 1024 * 1024),
        name='decode_layer',
    )(*in_hbm, w_qkv, w_out, w_up, w_down, k_cache, v_cache, pltpu.with_memory_space_constraint(positions, pltpu.HBM), inv_freq.reshape(1, -1))
    return pl.pallas_call(
        store_kernel,
        out_shape=[jax.ShapeDtypeStruct(r.shape, r.dtype) for r in results],
        in_specs=[vmem_spec] * 3,
        out_specs=[pl.BlockSpec(memory_space=pltpu.HBM)] * 3,
        scratch_shapes=[dma((3, 4))],
        compiler_params=pltpu.CompilerParams(vmem_limit_bytes=1024 * 1024),
        name='store_results',
    )(*results)


def solution(mesh):
    rows, cache = P('dp'), P('dp', 'sp')
    in_specs = (rows, P(), P(), P(), P(), P(None, 'sp'), P('sp'), cache, cache, rows)
    out_specs = (rows, cache, cache)
    return jax.shard_map(functools.partial(device_step, mesh.shape['sp']), mesh=mesh, in_specs=in_specs, out_specs=out_specs, check_vma=False)
```
